512 devices in a mesh: wide: 64 (over z, y), narrow: 8 (over x, core).
Axes of the slice: x: 4, y: 4, z: 16, core: 2. Of those that a mesh axis runs over, the one named last changes fastest.
Arguments:
- query_coords: float32 [3, 512, 16, 512], P(None, ('wide', 'narrow')), may hold values from -1 to 1
- owner_element: int32 [512, 16, 512], P(('wide', 'narrow')), may hold values from 0 to 15
- pair_counts: int32 [512, 512], P(('wide', 'narrow')), may hold values from 0 to 16, as said below
- fields: bfloat16 [8192, 8, 1024], P(('wide', 'narrow')), may hold values from -6 to 6
Outputs:
- values: bfloat16 [16, 512, 16, 512], P(None, ('wide', 'narrow'))
The draws below stay inside these ranges and needn't reach their ends.
Inputs may be any that keep to these rules, and one draw needn't show every extreme that they name: `pair_counts`: every count is at most 16, and some pair of devices reaches 16 in every draw.
All inputs are finite; a program needn't handle non-finite values.
Results may differ from the reference program's by a relative error of at most 0.0043.
Values may be sent and summed in bfloat16 or wider, within the bound.
A program may use at most 64 MiB of HBM per device.

```python
import jax
import jax.numpy as jnp
from jax import lax

FIELDS = 16
NODE = 8
E_DEV = 16
CAP = 16
ELEMS = 8192
DEVICES = 512


def draw_pair_counts(key, part):
    key_shift, key_hot, key_count, key_sender = jax.random.split(key, 4)
    shifts = jax.random.randint(key_shift, (DEVICES,), 0, 2)
    hottest = jax.random.randint(key_hot, (), 0, DEVICES)
    owners = jnp.arange(DEVICES)
    shifts = jnp.where(owners == hottest, 0, shifts)
    limits = jnp.maximum(jnp.right_shift(jnp.full((DEVICES,), CAP, jnp.int32), shifts.astype(jnp.int32)), 1)
    lowest = limits // 2
    raw_bits = jax.random.randint(key_count, (DEVICES, DEVICES), 0, 1 << 20)
    counts = lowest[None, :] + raw_bits % (limits[None, :] - lowest[None, :] + 1)
    sender = jax.random.randint(key_sender, (), 0, DEVICES)
    senders = jnp.arange(DEVICES)
    counts = jnp.where((senders[:, None] == sender) & (owners[None, :] == hottest), CAP, counts)
    return counts.astype(jnp.int32)


def with_ends(array, stream_key, low, high):
    spot = [jax.random.randint(jax.random.fold_in(stream_key, axis), (), 0, length) for axis, length in enumerate(array.shape)]
    longest = array.shape.index(max(array.shape))
    beside = spot[:longest] + [(spot[longest] + 1) % array.shape[longest]] + spot[longest + 1:]
    return array.at[tuple(spot)].set(low).at[tuple(beside)].set(high)


def shard_levels(own_key, extent, pieces, smallest, top_value):
    def one(axis_at, blocks):
        steps = jax.random.uniform(jax.random.fold_in(jax.random.fold_in(own_key, 6), axis_at), (blocks,), jnp.float32, smallest / len(pieces), top_value / len(pieces))
        return jnp.repeat(jnp.exp(steps), extent[axis_at] // blocks).reshape((-1,) + (1,) * (len(extent) - axis_at - 1))

    level = one(*pieces[0])
    for cut in pieces[1:]:
        level = level * one(*cut)
    return level


def centred(own_key, shape, spread, reach, cuts=(), kind=jnp.bfloat16):
    array = spread * jax.random.normal(own_key, shape, jnp.float32)
    if cuts:
        array = array * shard_levels(own_key, shape, cuts, -0.22, 0.18)
    return jnp.clip(array, -reach, reach).astype(kind)


def setup_inputs(seed: int = 0) -> dict:
    seeds = jax.random.split(jax.random.key(seed), 5)
    return {
        "query_coords": jnp.clip(jax.random.uniform(seeds[0], (3, DEVICES, CAP, DEVICES), jnp.float32, -1.0, 1.0) * shard_levels(seeds[0], (3, DEVICES, CAP, DEVICES), ((1, 512),), -0.4, 0.0), -1.0, 1.0),
        "owner_element": with_ends(jax.random.randint(seeds[1], (DEVICES, CAP, DEVICES), 0, E_DEV), jax.random.fold_in(seeds[1], 1), 0, E_DEV - 1).astype(jnp.int32),
        "pair_counts": draw_pair_counts(jax.random.fold_in(seeds[4], 71), 0),
        "fields": centred(seeds[3], (ELEMS, NODE, FIELDS * NODE * NODE), 1.0, 6.0, ((0, 512),)),
    }


GLL_NODES = (-1.0, -0.8717401485096066, -0.5917001814331423, -0.2092992179024789, 0.2092992179024789, 0.5917001814331423, 0.8717401485096066, 1.0)


def lagrange(position):
    result = []
    for i in range(8):
        factor = jnp.ones_like(position)
        for m in range(8):
            if m != i:
                factor = factor * ((position - GLL_NODES[m]) / (GLL_NODES[i] - GLL_NODES[m]))
        result.append(factor)
    return jnp.stack(result)


def reference(query_coords, owner_element, pair_counts, fields):
    field_table = fields.reshape(DEVICES, E_DEV, NODE, FIELDS * NODE * NODE)

    def one_owner(owner_index):
        coords_here = lax.dynamic_index_in_dim(query_coords, owner_index, 3, keepdims=False)
        element_here = lax.dynamic_index_in_dim(owner_element, owner_index, 2, keepdims=False)
        counts_here = lax.dynamic_index_in_dim(pair_counts, owner_index, 1, keepdims=False)
        owned = lax.dynamic_index_in_dim(field_table, owner_index, 0, keepdims=False)

        def one_slot(slot_index):
            picked_coords = lax.dynamic_index_in_dim(coords_here, slot_index, 2, keepdims=False)
            element_ids = lax.dynamic_index_in_dim(element_here, slot_index, 1, keepdims=False)
            live = slot_index < counts_here
            basis_r = lagrange(picked_coords[0]).astype(jnp.bfloat16).astype(jnp.float32)
            tensor_st = (lagrange(picked_coords[1])[:, None, :] * lagrange(picked_coords[2])[None, :, :]).reshape(NODE * NODE, -1)
            gathered = owned[element_ids].astype(jnp.float32)
            partial_value = jnp.einsum('sin,is->sn', gathered, basis_r)
            summed = jnp.sum(partial_value.reshape(-1, FIELDS, NODE * NODE) * tensor_st.T[:, None, :], axis=-1)
            return jnp.where(live[:, None], summed, jnp.float32(0.0)).astype(jnp.bfloat16).T

        return lax.map(one_slot, jnp.arange(CAP, dtype=jnp.int32))

    stacked = lax.map(one_owner, jnp.arange(DEVICES, dtype=jnp.int32))
    return jnp.transpose(stacked, (2, 3, 1, 0))
```

```python
import functools

import jax
import jax.numpy as jnp
from jax import lax
from jax.experimental import pallas as pl
from jax.experimental.pallas import tpu as pltpu
from jax.sharding import PartitionSpec as P

GLL_NODES = (
    -1.0,
    -0.8717401485096066,
    -0.5917001814331423,
    -0.2092992179024789,
    0.2092992179024789,
    0.5917001814331423,
    0.8717401485096066,
    1.0,
)
MESH = pl.DeviceIdType.MESH
NZ = 16
NQ = 32
NY = 4
NX = 8


def node_constants():
    rows = []
    scale = []
    for i in range(8):
        product = 1.0
        for m in range(8):
            if m != i:
                product *= GLL_NODES[i] - GLL_NODES[m]
        scale.append(1.0 / product)
    rows.append(scale)
    for k in range(1, 8):
        rows.append([GLL_NODES[(i + k) % 8] for i in range(8)])
    return rows


def sublane_constant(values):
    index = lax.broadcasted_iota(jnp.int32, (8, 128), 0)
    result = jnp.full((8, 128), values[0], jnp.float32)
    for i in range(1, 8):
        result = jnp.where(index == i, jnp.float32(values[i]), result)
    return result


def lagrange(position, consts):
    result = consts[0]
    for k in range(1, 8):
        result = result * (position - consts[k])
    return result


def encode(x):
    return (x * 32767.0 + 32768.5).astype(jnp.int32)


def decode(u):
    return (u - 32768).astype(jnp.float32) * jnp.float32(1.0 / 32767.0)


def kernel(
    qc, oe, pc, fl, out,
    ft, gf, ee, sq, rq, sz, rz, ts, vs, rv, srf, sr, rr, orf,
    qs_sem, qr_sem, zs_sem, zr_sem, vs_sem, vr_sem, ws_sem, wr_sem,
):
    wide = lax.axis_index("wide")
    narrow = lax.axis_index("narrow")
    z = wide // NY
    y = wide % NY
    q = y * NX + narrow

    def plane_peer(k):
        peer = (q + k) % NQ
        return peer, (z * NY + peer // NX, peer % NX)

    def z_peer(k):
        peer = (z + k) % NZ
        return peer, (peer * NY + y, narrow)

    barrier = pltpu.get_barrier_semaphore()

    def greet_plane(k, carry):
        pl.semaphore_signal(barrier, inc=1, device_id=plane_peer(k)[1], device_id_type=MESH)
        return carry

    def greet_z(k, carry):
        pl.semaphore_signal(barrier, inc=1, device_id=z_peer(k)[1], device_id_type=MESH)
        return carry

    lax.fori_loop(1, NZ, greet_z, 0)
    lax.fori_loop(1, NQ, greet_plane, 0)

    for h in range(4):
        rows = pl.ds(4 * h, 4)
        slot = lax.broadcasted_iota(jnp.int32, (4, 512), 0) + 4 * h
        live = slot < pc[0:1, :]
        element = jnp.where(live, oe[0, rows, :], 16)
        ee[h, 0:4, :] = jnp.left_shift(encode(qc[0, 0, rows, :]), 16) + encode(qc[1, 0, rows, :])
        ee[h, 4:8, :] = jnp.left_shift(encode(qc[2, 0, rows, :]), 16) + element
    group = lax.broadcasted_iota(jnp.int32, (8, 128), 1) // 32
    blocks = []
    for t in range(4):
        pieces = [ee[h, :, t * 128 : (t + 1) * 128] for h in range(4)]
        for zl in range(4):
            block = None
            for h in range(4):
                shift = ((h - zl) * 32) % 128
                piece = pieces[h] if shift == 0 else pltpu.roll(pieces[h], shift, 1)
                block = piece if block is None else jnp.where(group == h, piece, block)
            blocks.append(block)
    turned = jnp.transpose(jnp.concatenate(blocks, axis=0))
    for h in range(4):
        sq[:, h, :] = turned[h * 32 : (h + 1) * 32, :]

    for b in range(8):
        part = fl[:, :, b * 128 : (b + 1) * 128].reshape(128, 128).astype(jnp.float32)
        gf[b * 128 : (b + 1) * 128, :] = jnp.transpose(part)

    def permute(n, carry):
        ft[pl.ds(pl.multiple_of(n * 16, 16), 16), :] = gf[pl.ds(n, 16, stride=64), :].astype(jnp.bfloat16)
        return carry

    lax.fori_loop(0, 64, permute, 0)
    consts = [sublane_constant(v) for v in node_constants()]

    pl.semaphore_wait(barrier, NQ - 1 + NZ - 1)

    def plane_copy(src, dst, send, recv, k):
        peer, device = plane_peer(k)
        return pltpu.make_async_remote_copy(
            src_ref=src.at[peer], dst_ref=dst.at[q], send_sem=send.at[peer], recv_sem=recv.at[q],
            device_id=device, device_id_type=MESH,
        )

    def plane_arrival(src, dst, send, recv, k):
        peer, device = plane_peer(k)
        return pltpu.make_async_remote_copy(
            src_ref=src.at[peer], dst_ref=dst.at[peer], send_sem=send.at[peer], recv_sem=recv.at[peer],
            device_id=device, device_id_type=MESH,
        )

    def z_copy(src, dst, send, recv, k):
        peer, device = z_peer(k)
        return pltpu.make_async_remote_copy(
            src_ref=src.at[peer], dst_ref=dst.at[z], send_sem=send.at[peer], recv_sem=recv.at[z],
            device_id=device, device_id_type=MESH,
        )

    def z_arrival(src, dst, send, recv, k):
        peer, device = z_peer(k)
        return pltpu.make_async_remote_copy(
            src_ref=src.at[peer], dst_ref=dst.at[peer], send_sem=send.at[peer], recv_sem=recv.at[peer],
            device_id=device, device_id_type=MESH,
        )

    def each(low, high, do):
        def step(k, carry):
            do(k)
            return carry

        lax.fori_loop(low, high, step, 0)

    each(1, NQ, lambda k: plane_copy(sq, rq, qs_sem, qr_sem, k).start())
    rq[pl.ds(q, 1)] = sq[pl.ds(q, 1)]
    each(1, NQ, lambda k: plane_arrival(sq, rq, qs_sem, qr_sem, k).wait_recv())
    gathered = jnp.concatenate([rq[:, h, :] for h in range(4)], axis=0)
    sz[...] = jnp.transpose(gathered).reshape(NZ, 8, 128)

    def far_first(k):
        n = NZ - k
        return ((n + 1) // 2 * (2 * (n % 2) - 1) + NZ) % NZ

    def near_first(k):
        return ((k + 1) // 2 * (2 * (k % 2) - 1) + NZ) % NZ

    each(1, NZ, lambda k: z_copy(sz, rz, zs_sem, zr_sem, far_first(k)).start())
    rz[pl.ds(z, 1)] = sz[pl.ds(z, 1)]

    def evaluate(peer):
        weights = []
        for sl in range(4):
            lanes = slice(sl * 128, (sl + 1) * 128)
            w0 = jnp.broadcast_to(rz[peer, sl : sl + 1, :], (8, 128))
            w1 = jnp.broadcast_to(rz[peer, 4 + sl : 5 + sl, :], (8, 128))
            basis_r = lagrange(decode(lax.shift_right_logical(w0, 16)), consts)
            basis_s = lagrange(decode(jnp.bitwise_and(w0, 65535)), consts)
            basis_t = lagrange(decode(lax.shift_right_logical(w1, 16)), consts)
            element = jnp.bitwise_and(w1, 65535)
            weights.append(
                jnp.concatenate(
                    [jnp.where(element == e, basis_r, 0.0) for e in range(16)], axis=0
                ).astype(jnp.bfloat16)
            )
            for j in range(8):
                ts[j * 8 : (j + 1) * 8, lanes] = basis_s[j : j + 1, :] * basis_t
        for half in range(2):
            pair = jnp.concatenate(weights[2 * half : 2 * half + 2], axis=1)
            lanes = slice(half * 256, (half + 1) * 256)
            partial = jnp.dot(ft[...], pair, preferred_element_type=jnp.float32)
            total = None
            for n in range(64):
                term = partial[n * 16 : (n + 1) * 16, :] * ts[n : n + 1, lanes]
                total = term if total is None else total + term
            rounded = total.astype(jnp.bfloat16)
            vs[peer, 2 * half] = rounded[:, :128]
            vs[peer, 2 * half + 1] = rounded[:, 128:]

    evaluate(z)
    rv[pl.ds(z, 1)] = vs[pl.ds(z, 1)]

    def remote_step(k, carry):
        offset = near_first(k)
        z_arrival(sz, rz, zs_sem, zr_sem, offset).wait_recv()
        evaluate((z + offset) % NZ)
        z_copy(vs, rv, vs_sem, vr_sem, offset).start()
        return carry

    lax.fori_loop(1, NZ, remote_step, 0)
    each(1, NZ, lambda k: z_arrival(vs, rv, vs_sem, vr_sem, near_first(k)).wait_recv())

    def turn_back(g, carry):
        zl = g // 2
        first = (g % 2) * 8 + zl
        both = jnp.concatenate(
            [rv[first].reshape(64, 128), rv[first + 4].reshape(64, 128)], axis=0
        ).astype(jnp.float32)
        rows = jnp.transpose(both)
        for h in range(4):
            srf[pl.ds(g * 4 + h, 32, stride=32), :] = rows[h * 32 : (h + 1) * 32, :]
        return carry

    lax.fori_loop(0, 8, turn_back, 0)

    def narrow_down(n, carry):
        sr[n] = srf[pl.ds(pl.multiple_of(n * 32, 32), 32), :].astype(jnp.bfloat16)
        return carry

    lax.fori_loop(0, NQ, narrow_down, 0)
    each(1, NQ, lambda k: plane_copy(sr, rr, ws_sem, wr_sem, k).start())
    rr[pl.ds(q, 1)] = sr[pl.ds(q, 1)]
    each(1, NQ, lambda k: plane_arrival(sr, rr, ws_sem, wr_sem, k).wait_recv())

    def widen(n, carry):
        srf[pl.ds(pl.multiple_of(n * 32, 32), 32), :] = rr[n].astype(jnp.float32)
        return carry

    lax.fori_loop(0, NQ, widen, 0)
    for t_hi in range(2):
        for h in range(4):
            rows = jnp.concatenate(
                [srf[pl.ds((zl * 2 + t_hi) * 4 + h, 32, stride=32), :] for zl in range(4)], axis=0
            )
            turned = jnp.transpose(rows)
            for t_lo in range(2):
                for sl in range(4):
                    at = t_lo * 64 + sl * 16
                    orf[2 * t_hi + t_lo, pl.ds(h * 4 + sl, 16, stride=16), :] = turned[at : at + 16, :]
    for t in range(4):
        for c in range(16):
            out[c, 0, :, t * 128 : (t + 1) * 128] = orf[t, c * 16 : (c + 1) * 16, :].astype(jnp.bfloat16)

    each(1, NQ, lambda k: plane_copy(sq, rq, qs_sem, qr_sem, k).wait_send())
    each(1, NZ, lambda k: z_copy(sz, rz, zs_sem, zr_sem, k).wait_send())
    each(1, NZ, lambda k: z_copy(vs, rv, vs_sem, vr_sem, k).wait_send())
    each(1, NQ, lambda k: plane_copy(sr, rr, ws_sem, wr_sem, k).wait_send())


def on_device(query_coords, owner_element, pair_counts, fields):
    vmem = pl.BlockSpec(memory_space=pltpu.VMEM)
    return pl.pallas_call(
        kernel,
        out_shape=jax.ShapeDtypeStruct((16, 1, 16, 512), jnp.bfloat16),
        in_specs=[vmem] * 4,
        out_specs=vmem,
        scratch_shapes=[
            pltpu.VMEM((1024, 128), jnp.bfloat16),
            pltpu.VMEM((1024, 128), jnp.float32),
            pltpu.VMEM((4, 8, 512), jnp.int32),
            pltpu.VMEM((NQ, 4, 128), jnp.int32),
            pltpu.VMEM((NQ, 4, 128), jnp.int32),
            pltpu.VMEM((NZ, 8, 128), jnp.int32),
            pltpu.VMEM((NZ, 8, 128), jnp.int32),
            pltpu.VMEM((64, 512), jnp.float32),
            pltpu.VMEM((NZ, 4, 16, 128), jnp.bfloat16),
            pltpu.VMEM((NZ, 4, 16, 128), jnp.bfloat16),
            pltpu.VMEM((NQ * 32, 128), jnp.float32),
            pltpu.VMEM((NQ, 32, 128), jnp.bfloat16),
            pltpu.VMEM((NQ, 32, 128), jnp.bfloat16),
            pltpu.VMEM((4, 256, 128), jnp.float32),
            pltpu.SemaphoreType.DMA((NQ,)),
            pltpu.SemaphoreType.DMA((NQ,)),
            pltpu.SemaphoreType.DMA((NZ,)),
            pltpu.SemaphoreType.DMA((NZ,)),
            pltpu.SemaphoreType.DMA((NZ,)),
            pltpu.SemaphoreType.DMA((NZ,)),
            pltpu.SemaphoreType.DMA((NQ,)),
            pltpu.SemaphoreType.DMA((NQ,)),
        ],
        compiler_params=pltpu.CompilerParams(collective_id=0, has_side_effects=True),
    )(query_coords, owner_element, pair_counts, fields)


def solution(mesh):
    placed = (
        P(None, ("wide", "narrow"), None, None),
        P(("wide", "narrow"), None, None),
        P(("wide", "narrow"), None),
        P(("wide", "narrow"), None, None),
    )
    return jax.shard_map(
        on_device,
        mesh=mesh,
        in_specs=placed,
        out_specs=P(None, ("wide", "narrow"), None, None),
        check_vma=False,
    )
```

```python
import functools

import jax
import jax.numpy as jnp
from jax import lax
from jax.experimental import pallas as pl
from jax.experimental.pallas import tpu as pltpu
from jax.sharding import PartitionSpec as P

GLL_NODES = (
    -1.0,
    -0.8717401485096066,
    -0.5917001814331423,
    -0.2092992179024789,
    0.2092992179024789,
    0.5917001814331423,
    0.8717401485096066,
    1.0,
)
MESH = pl.DeviceIdType.MESH
NZ = 16
NQ = 32
NY = 4
NX = 8
NEAR = 10
GROUPS = 4


def node_constants():
    rows = []
    scale = []
    for i in range(8):
        product = 1.0
        for m in range(8):
            if m != i:
                product *= GLL_NODES[i] - GLL_NODES[m]
        scale.append(1.0 / product)
    rows.append(scale)
    for k in range(1, 8):
        rows.append([GLL_NODES[(i + k) % 8] for i in range(8)])
    return rows


def sublane_constant(values):
    index = lax.broadcasted_iota(jnp.int32, (8, 128), 0)
    result = jnp.full((8, 128), values[0], jnp.float32)
    for i in range(1, 8):
        result = jnp.where(index == i, jnp.float32(values[i]), result)
    return result


def lagrange(position, consts):
    result = consts[0]
    for k in range(1, 8):
        result = result * (position - consts[k])
    return result


def encode(x):
    return (x * 32767.0 + 32768.5).astype(jnp.int32)


def decode(u):
    return (u - 32768).astype(jnp.float32) * jnp.float32(1.0 / 32767.0)


def position_to_nearness(k):
    late = lax.div(k + 15 - NEAR, 16)
    return k * (1 - late) + (NZ + NEAR - k) * late


def nearness_to_offset(n):
    return lax.rem(lax.div(n + 1, 2) * (2 * lax.rem(n, 2) - 1) + NZ, NZ)


def offset_to_position(o):
    side = lax.div(o + 7, 16)
    n = (2 * o - lax.div(o + 15, 16)) * (1 - side) + (2 * NZ - 2 * o) * side
    return position_to_nearness(n)


def each(low, high, do):
    def step(k, carry):
        do(k)
        return carry

    lax.fori_loop(low, high, step, 0)


def kernel(
    qc_hbm, oe_hbm, pc_hbm, fl_hbm, rr,
    qc, oe, pc, fl, ft, gf, ee, sq, rq, sz, rz, ts, vs, rv, srf, sr,
    in_sem, qs_sem, qr_sem, zs_sem, zr_sem, vs_sem, vr_sem, ws_sem, wr_sem, own_sem,
):
    wide = lax.axis_index("wide")
    narrow = lax.axis_index("narrow")
    z = lax.div(wide, NY)
    y = lax.rem(wide, NY)
    q = y * NX + narrow

    def plane_peer(k):
        peer = lax.rem(q + k, NQ)
        return peer, (z * NY + lax.div(peer, NX), lax.rem(peer, NX))

    def z_peer(o):
        peer = lax.rem(z + o, NZ)
        return peer, (peer * NY + y, narrow)

    loads = [
        pltpu.make_async_copy(src, dst, in_sem.at[n])
        for n, (src, dst) in enumerate(((qc_hbm, qc), (oe_hbm, oe), (pc_hbm, pc), (fl_hbm, fl)))
    ]
    barrier = pltpu.get_barrier_semaphore()

    def greet_plane(k):
        pl.semaphore_signal(barrier, inc=1, device_id=plane_peer(k)[1], device_id_type=MESH)

    def greet_z(k):
        device = z_peer(nearness_to_offset(NZ - k))[1]
        pl.semaphore_signal(barrier, inc=1, device_id=device, device_id_type=MESH)

    with jax.named_scope("greet"):
        for load in loads:
            load.start()
        each(1, NZ, greet_z)
        each(1, NQ, greet_plane)

    with jax.named_scope("load"):
        for load in loads[:3]:
            load.wait()

    with jax.named_scope("encode"):
        for h in range(4):
            rows = pl.ds(4 * h, 4)
            slot = lax.broadcasted_iota(jnp.int32, (4, 512), 0) + 4 * h
            live = slot < pc[0:1, :]
            element = jnp.where(live, oe[0, rows, :], 16)
            ee[h, 0:4, :] = jnp.left_shift(encode(qc[0, 0, rows, :]), 16) + encode(qc[1, 0, rows, :])
            ee[h, 4:8, :] = jnp.left_shift(encode(qc[2, 0, rows, :]), 16) + element
        group = lax.broadcasted_iota(jnp.int32, (8, 128), 1) // 32
        blocks = []
        for t in range(4):
            pieces = [ee[h, :, t * 128 : (t + 1) * 128] for h in range(4)]
            for zl in range(4):
                block = None
                for h in range(4):
                    shift = ((h - zl) * 32) % 128
                    piece = pieces[h] if shift == 0 else pltpu.roll(pieces[h], shift, 1)
                    block = piece if block is None else jnp.where(group == h, piece, block)
                blocks.append(block)
        turned = jnp.transpose(jnp.concatenate(blocks, axis=0))
        for h in range(4):
            sq[:, h, :] = turned[h * 32 : (h + 1) * 32, :]

    with jax.named_scope("barrier"):
        pl.semaphore_wait(barrier, NQ - 1 + NZ - 1)

    def plane_copy(src, dst, send, recv, k):
        peer, device = plane_peer(k)
        return pltpu.make_async_remote_copy(
            src_ref=src.at[peer], dst_ref=dst.at[q], send_sem=send, recv_sem=recv,
            device_id=device, device_id_type=MESH,
        )

    def plane_all(src, dst, send, recv):
        others = pl.ds(0, NQ - 1)
        return pltpu.make_async_remote_copy(
            src_ref=src.at[others], dst_ref=dst.at[others], send_sem=send, recv_sem=recv,
            device_id=plane_peer(1)[1], device_id_type=MESH,
        )

    def z_copy(src, dst, send, recv, o):
        peer, device = z_peer(o)
        return pltpu.make_async_remote_copy(
            src_ref=src.at[peer], dst_ref=dst.at[z], send_sem=send, recv_sem=recv.at[z],
            device_id=device, device_id_type=MESH,
        )

    def z_arrival(src, dst, send, recv, o):
        peer, device = z_peer(o)
        return pltpu.make_async_remote_copy(
            src_ref=src.at[peer], dst_ref=dst.at[peer], send_sem=send, recv_sem=recv.at[peer],
            device_id=device, device_id_type=MESH,
        )

    def z_all(src, dst, send, recv):
        others = pl.ds(0, NZ - 1)
        return pltpu.make_async_remote_copy(
            src_ref=src.at[others], dst_ref=dst.at[others], send_sem=send, recv_sem=recv.at[0],
            device_id=z_peer(1)[1], device_id_type=MESH,
        )

    with jax.named_scope("plane_send"):
        each(1, NQ, lambda k: plane_copy(sq, rq, qs_sem.at[0], qr_sem.at[0], k).start())
        rq[pl.ds(q, 1)] = sq[pl.ds(q, 1)]

    def permute(n):
        ft[pl.ds(pl.multiple_of(n * 16, 16), 16), :] = gf[pl.ds(n, 16, stride=64), :].astype(jnp.bfloat16)

    with jax.named_scope("table"):
        loads[3].wait()
        for b in range(8):
            part = fl[:, :, b * 128 : (b + 1) * 128].reshape(128, 128).astype(jnp.float32)
            gf[b * 128 : (b + 1) * 128, :] = jnp.transpose(part)
        each(0, 64, permute)
    consts = [sublane_constant(v) for v in node_constants()]

    with jax.named_scope("plane_wait"):
        plane_all(sq, rq, qs_sem.at[0], qr_sem.at[0]).wait_recv()
    with jax.named_scope("turn_queries"):
        gathered = jnp.concatenate([rq[:, h, :] for h in range(4)], axis=0)
        sz[...] = jnp.transpose(gathered).reshape(NZ, 8, 128)

    with jax.named_scope("z_send"):
        each(1, NZ, lambda k: z_copy(sz, rz, zs_sem.at[0], zr_sem, nearness_to_offset(k)).start())
        rz[pl.ds(z, 1)] = sz[pl.ds(z, 1)]

    def evaluate(peer):
        weights = []
        for sl in range(4):
            lanes = slice(sl * 128, (sl + 1) * 128)
            w0 = jnp.broadcast_to(rz[peer, sl : sl + 1, :], (8, 128))
            w1 = jnp.broadcast_to(rz[peer, 4 + sl : 5 + sl, :], (8, 128))
            basis_r = lagrange(decode(lax.shift_right_logical(w0, 16)), consts)
            basis_s = lagrange(decode(jnp.bitwise_and(w0, 65535)), consts)
            basis_t = lagrange(decode(lax.shift_right_logical(w1, 16)), consts)
            element = jnp.bitwise_and(w1, 65535)
            weights.append(
                jnp.concatenate(
                    [jnp.where(element == e, basis_r, 0.0) for e in range(16)], axis=0
                ).astype(jnp.bfloat16)
            )
            for j in range(8):
                ts[j * 8 : (j + 1) * 8, lanes] = basis_s[j : j + 1, :] * basis_t
        for half in range(2):
            pair = jnp.concatenate(weights[2 * half : 2 * half + 2], axis=1)
            lanes = slice(half * 256, (half + 1) * 256)
            partial = jnp.dot(ft[...], pair, preferred_element_type=jnp.float32)
            total = None
            for n in range(64):
                term = partial[n * 16 : (n + 1) * 16, :] * ts[n : n + 1, lanes]
                total = term if total is None else total + term
            rounded = total.astype(jnp.bfloat16)
            vs[peer, 2 * half] = rounded[:, :128]
            vs[peer, 2 * half + 1] = rounded[:, 128:]

    with jax.named_scope("own"):
        evaluate(z)
        rv[pl.ds(z, 1)] = vs[pl.ds(z, 1)]

    def remote_step(k):
        offset = nearness_to_offset(position_to_nearness(k))
        with jax.named_scope("z_wait"):
            z_arrival(sz, rz, zs_sem.at[0], zr_sem, offset).wait_recv()
        with jax.named_scope("evaluate"):
            evaluate(lax.rem(z + offset, NZ))
            z_copy(vs, rv, vs_sem.at[0], vr_sem, offset).start()

    each(1, NZ, remote_step)

    def turn_back(n, at):
        offset = nearness_to_offset(position_to_nearness(n))
        block = rv[lax.rem(z + offset, NZ)].reshape(64, 128).astype(jnp.float32)
        rows = jnp.transpose(jnp.concatenate([block, pltpu.roll(block, 96, 1)], axis=0))
        for half in range(2):
            srf[pl.ds(2 * at + half, 32, stride=8), :] = rows[half * 64 : half * 64 + 32, :]

    def return_group(g, first):
        def wait(n):
            offset = nearness_to_offset(position_to_nearness(n))
            z_arrival(vs, rv, vs_sem.at[0], vr_sem, offset).wait_recv()

        with jax.named_scope("z_return"):
            each(first, 4 * g + 4, wait)
        with jax.named_scope("turn_back"):
            for at in range(4):
                turn_back(4 * g + at, at)
            sr[g] = srf[...].reshape(NQ, 8, 128).astype(jnp.bfloat16)
        with jax.named_scope("plane_return"):
            each(1, NQ, lambda k: plane_copy(sr.at[g], rr.at[g], ws_sem.at[g], wr_sem.at[g], k).start())
            pltpu.make_async_copy(sr.at[g, q], rr.at[g, q], own_sem.at[g]).start()

    for g in range(GROUPS):
        return_group(g, max(4 * g, 1))
    with jax.named_scope("drain"):
        plane_all(sq, rq, qs_sem.at[0], qr_sem.at[0]).wait_send()
        z_all(sz, rz, zs_sem.at[0], zr_sem).wait_send()
        z_all(vs, rv, vs_sem.at[0], vr_sem).wait_send()
    with jax.named_scope("plane_back"):
        for g in range(GROUPS):
            plane_all(sr.at[g], rr.at[g], ws_sem.at[g], wr_sem.at[g]).wait_recv()
            pltpu.make_async_copy(sr.at[g, q], rr.at[g, q], own_sem.at[g]).wait()
    with jax.named_scope("drain2"):
        for g in range(GROUPS):
            plane_all(sr.at[g], rr.at[g], ws_sem.at[g], wr_sem.at[g]).wait_send()


def finish(rr_hbm, out_hbm, rr, srf, orf, staged, sem, in_sem):
    loads = [pltpu.make_async_copy(rr_hbm.at[g], rr.at[g], in_sem.at[g]) for g in range(GROUPS)]
    for load in loads:
        load.start()
    z = lax.div(lax.axis_index("wide"), NY)

    with jax.named_scope("widen"):
        for g in range(GROUPS):
            loads[g].wait()
            srf[g] = rr[g].reshape(NQ * 8, 128).astype(jnp.float32)
    copies = []
    for t in range(4):
        with jax.named_scope("finish"):
            for half in range(2):
                parts = []
                for zl in range(4):
                    position = offset_to_position(lax.rem(t * 4 + zl - z + NZ, NZ))
                    row = lax.rem(position, 4) * 2 + half
                    parts.append(srf[lax.div(position, 4), pl.ds(row, 32, stride=8), :])
                turned = jnp.transpose(jnp.concatenate(parts, axis=0))
                for n in range(8):
                    orf[t, pl.ds(half * 8 + n, 16, stride=16), :] = turned[n * 16 : (n + 1) * 16, :]
            staged[t] = orf[t].reshape(16, 16, 128).astype(jnp.bfloat16)
            copy = pltpu.make_async_copy(
                staged.at[t], out_hbm.at[:, 0, :, pl.ds(t * 128, 128)], sem.at[t]
            )
            copy.start()
            copies.append(copy)
    with jax.named_scope("store"):
        for copy in copies:
            copy.wait()


def on_device(query_coords, owner_element, pair_counts, fields):
    anywhere = pl.BlockSpec(memory_space=pl.ANY)
    vmem = pl.BlockSpec(memory_space=pltpu.VMEM)
    returned = pl.pallas_call(
        kernel,
        out_shape=jax.ShapeDtypeStruct((GROUPS, NQ, 8, 128), jnp.bfloat16),
        in_specs=[anywhere] * 4,
        out_specs=anywhere,
        scratch_shapes=[
            pltpu.VMEM((3, 1, 16, 512), jnp.float32),
            pltpu.VMEM((1, 16, 512), jnp.int32),
            pltpu.VMEM((1, 512), jnp.int32),
            pltpu.VMEM((16, 8, 1024), jnp.bfloat16),
            pltpu.VMEM((1024, 128), jnp.bfloat16),
            pltpu.VMEM((1024, 128), jnp.float32),
            pltpu.VMEM((4, 8, 512), jnp.int32),
            pltpu.VMEM((NQ, 4, 128), jnp.int32),
            pltpu.VMEM((NQ, 4, 128), jnp.int32),
            pltpu.VMEM((NZ, 8, 128), jnp.int32),
            pltpu.VMEM((NZ, 8, 128), jnp.int32),
            pltpu.VMEM((64, 512), jnp.float32),
            pltpu.VMEM((NZ, 4, 16, 128), jnp.bfloat16),
            pltpu.VMEM((NZ, 4, 16, 128), jnp.bfloat16),
            pltpu.VMEM((NQ * 8, 128), jnp.float32),
            pltpu.VMEM((GROUPS, NQ, 8, 128), jnp.bfloat16),
            pltpu.SemaphoreType.DMA((4,)),
            pltpu.SemaphoreType.DMA((1,)),
            pltpu.SemaphoreType.DMA((1,)),
            pltpu.SemaphoreType.DMA((1,)),
            pltpu.SemaphoreType.DMA((NZ,)),
            pltpu.SemaphoreType.DMA((1,)),
            pltpu.SemaphoreType.DMA((NZ,)),
            pltpu.SemaphoreType.DMA((GROUPS,)),
            pltpu.SemaphoreType.DMA((GROUPS,)),
            pltpu.SemaphoreType.DMA((GROUPS,)),
        ],
        compiler_params=pltpu.CompilerParams(collective_id=0, has_side_effects=True),
    )(query_coords, owner_element, pair_counts, fields)
    return pl.pallas_call(
        finish,
        out_shape=jax.ShapeDtypeStruct((16, 1, 16, 512), jnp.bfloat16),
        in_specs=[anywhere],
        out_specs=anywhere,
        scratch_shapes=[
            pltpu.VMEM((GROUPS, NQ, 8, 128), jnp.bfloat16),
            pltpu.VMEM((GROUPS, NQ * 8, 128), jnp.float32),
            pltpu.VMEM((4, 256, 128), jnp.float32),
            pltpu.VMEM((4, 16, 16, 128), jnp.bfloat16),
            pltpu.SemaphoreType.DMA((4,)),
            pltpu.SemaphoreType.DMA((GROUPS,)),
        ],
    )(returned)


def solution(mesh):
    placed = (
        P(None, ("wide", "narrow"), None, None),
        P(("wide", "narrow"), None, None),
        P(("wide", "narrow"), None),
        P(("wide", "narrow"), None, None),
    )
    return jax.shard_map(
        on_device,
        mesh=mesh,
        in_specs=placed,
        out_specs=P(None, ("wide", "narrow"), None, None),
        check_vma=False,
    )
```

```python
import functools

import jax
import jax.numpy as jnp
from jax import lax
from jax.experimental import pallas as pl
from jax.experimental.pallas import tpu as pltpu
from jax.sharding import PartitionSpec as P

GLL_NODES = (
    -1.0,
    -0.8717401485096066,
    -0.5917001814331423,
    -0.2092992179024789,
    0.2092992179024789,
    0.5917001814331423,
    0.8717401485096066,
    1.0,
)
LOGICAL = pl.DeviceIdType.LOGICAL
NZ = 16
NQ = 32
NY = 4
NX = 8
NEAR = 10
GROUPS = 4


def node_constants():
    rows = []
    scale = []
    for i in range(8):
        product = 1.0
        for m in range(8):
            if m != i:
                product *= GLL_NODES[i] - GLL_NODES[m]
        scale.append(1.0 / product)
    rows.append(scale)
    for k in range(1, 8):
        rows.append([GLL_NODES[(i + k) % 8] for i in range(8)])
    return rows


def sublane_constant(values):
    index = lax.broadcasted_iota(jnp.int32, (8, 128), 0)
    result = jnp.full((8, 128), values[0], jnp.float32)
    for i in range(1, 8):
        result = jnp.where(index == i, jnp.float32(values[i]), result)
    return result


def lagrange(position, consts):
    result = consts[0]
    for k in range(1, 8):
        result = result * (position - consts[k])
    return result


def encode(x):
    return (x * 32767.0 + 32768.5).astype(jnp.int32)


def decode(u):
    return (u - 32768).astype(jnp.float32) * jnp.float32(1.0 / 32767.0)


def position_to_nearness(k):
    late = lax.div(k + 15 - NEAR, 16)
    return k * (1 - late) + (NZ + NEAR - k) * late


def nearness_to_offset(n):
    return lax.rem(lax.div(n + 1, 2) * (1 - 2 * lax.rem(n, 2)) + NZ, NZ)


def offset_to_position(o):
    o = lax.rem(NZ - o, NZ)
    side = lax.div(o + 7, 16)
    n = (2 * o - lax.div(o + 15, 16)) * (1 - side) + (2 * NZ - 2 * o) * side
    return position_to_nearness(n)


def each(low, high, do):
    def step(k, carry):
        do(k)
        return carry

    lax.fori_loop(low, high, step, 0)


def kernel(
    qc_hbm, oe_hbm, pc_hbm, fl_hbm, rr,
    qc, oe, pc, fl, ft, gf, ee, sq, rq, sz, rz, ts, vs, rv, srf, sr,
    in_sem, qs_sem, qr_sem, zs_sem, zr_sem, vs_sem, vr_sem, ws_sem, wr_sem, own_sem, told,
):
    wide = lax.axis_index("wide")
    narrow = lax.axis_index("narrow")
    z = lax.div(wide, NY)
    q = lax.rem(wide, NY) * NX + narrow
    me = z * NQ + q
    core = lax.rem(narrow, 2)

    def plane_peer(k):
        peer = lax.rem(q + k, NQ)
        return peer, z * NQ + peer

    def z_peer(o):
        peer = lax.rem(z + o, NZ)
        return peer, peer * NQ + q

    loads = [
        pltpu.make_async_copy(src, dst, in_sem.at[n])
        for n, (src, dst) in enumerate(((qc_hbm, qc), (oe_hbm, oe), (pc_hbm, pc), (fl_hbm, fl)))
    ]
    barrier = pltpu.get_barrier_semaphore()

    def greet_plane(k):
        chip = lax.rem(lax.div(q, 2) + k, NQ // 2)
        pl.semaphore_signal(barrier, inc=1, device_id=z * NQ + 2 * chip, device_id_type=LOGICAL)

    def greet_z(k):
        peer = z_peer(nearness_to_offset(NZ - k))[1]
        pl.semaphore_signal(barrier, inc=1, device_id=peer - core + 1, device_id_type=LOGICAL)

    with jax.named_scope("greet"):
        for load in loads:
            load.start()
        each(1, NZ, greet_z)
        each(1, NQ // 2, greet_plane)

        @pl.when(core == 1)
        def _():
            pl.semaphore_signal(barrier, inc=1, device_id=me - 1, device_id_type=LOGICAL)

    with jax.named_scope("load"):
        for load in loads[:3]:
            load.wait()

    with jax.named_scope("encode"):
        for h in range(4):
            rows = pl.ds(4 * h, 4)
            slot = lax.broadcasted_iota(jnp.int32, (4, 512), 0) + 4 * h
            live = slot < pc[0:1, :]
            element = jnp.where(live, oe[0, rows, :], 16)
            ee[h, 0:4, :] = jnp.left_shift(encode(qc[0, 0, rows, :]), 16) + encode(qc[1, 0, rows, :])
            ee[h, 4:8, :] = jnp.left_shift(encode(qc[2, 0, rows, :]), 16) + element
        group = lax.broadcasted_iota(jnp.int32, (8, 128), 1) // 32
        blocks = []
        for t in range(4):
            pieces = [ee[h, :, t * 128 : (t + 1) * 128] for h in range(4)]
            for zl in range(4):
                block = None
                for h in range(4):
                    shift = ((h - zl) * 32) % 128
                    piece = pieces[h] if shift == 0 else pltpu.roll(pieces[h], shift, 1)
                    block = piece if block is None else jnp.where(group == h, piece, block)
                blocks.append(block)
        turned = jnp.transpose(jnp.concatenate(blocks, axis=0))
        for h in range(4):
            sq[:, h, :] = turned[h * 32 : (h + 1) * 32, :]

    with jax.named_scope("barrier"):

        @pl.when(core == 0)
        def _():
            pl.semaphore_wait(barrier, NQ - 1)
            pl.semaphore_signal(told, inc=1, device_id=me + 1, device_id_type=LOGICAL)

        @pl.when(core == 1)
        def _():
            pl.semaphore_wait(told, 1)

    def plane_copy(src, dst, send, recv, k):
        peer, device = plane_peer(k)
        return pltpu.make_async_remote_copy(
            src_ref=src.at[peer], dst_ref=dst.at[q], send_sem=send, recv_sem=recv,
            device_id=device, device_id_type=LOGICAL,
        )

    def plane_all(src, dst, send, recv):
        others = pl.ds(0, NQ - 1)
        return pltpu.make_async_remote_copy(
            src_ref=src.at[others], dst_ref=dst.at[others], send_sem=send, recv_sem=recv,
            device_id=plane_peer(1)[1], device_id_type=LOGICAL,
        )

    def z_copy(src, dst, send, recv, o):
        peer, device = z_peer(o)
        return pltpu.make_async_remote_copy(
            src_ref=src.at[peer], dst_ref=dst.at[z], send_sem=send, recv_sem=recv.at[z],
            device_id=device, device_id_type=LOGICAL,
        )

    def z_arrival(src, dst, send, recv, o):
        peer, device = z_peer(o)
        return pltpu.make_async_remote_copy(
            src_ref=src.at[peer], dst_ref=dst.at[peer], send_sem=send, recv_sem=recv.at[peer],
            device_id=device, device_id_type=LOGICAL,
        )

    def z_all(src, dst, send, recv):
        others = pl.ds(0, NZ - 1)
        return pltpu.make_async_remote_copy(
            src_ref=src.at[others], dst_ref=dst.at[others], send_sem=send, recv_sem=recv.at[0],
            device_id=z_peer(1)[1], device_id_type=LOGICAL,
        )

    with jax.named_scope("plane_send"):
        each(1, NQ, lambda k: plane_copy(sq, rq, qs_sem.at[0], qr_sem.at[0], k).start())
        rq[pl.ds(q, 1)] = sq[pl.ds(q, 1)]

    def permute(n):
        ft[pl.ds(pl.multiple_of(n * 16, 16), 16), :] = gf[pl.ds(n, 16, stride=64), :].astype(jnp.bfloat16)

    with jax.named_scope("table"):
        loads[3].wait()
        for b in range(8):
            part = fl[:, :, b * 128 : (b + 1) * 128].reshape(128, 128).astype(jnp.float32)
            gf[b * 128 : (b + 1) * 128, :] = jnp.transpose(part)
        each(0, 64, permute)
    consts = [sublane_constant(v) for v in node_constants()]

    with jax.named_scope("barrier_z"):

        @pl.when(core == 1)
        def _():
            pl.semaphore_wait(barrier, 2 * (NZ - 1))
            pl.semaphore_signal(told, inc=1, device_id=me - 1, device_id_type=LOGICAL)

        @pl.when(core == 0)
        def _():
            pl.semaphore_wait(told, 1)

    with jax.named_scope("plane_wait"):
        plane_all(sq, rq, qs_sem.at[0], qr_sem.at[0]).wait_recv()
    with jax.named_scope("turn_queries"):
        gathered = jnp.concatenate([rq[:, h, :] for h in range(4)], axis=0)
        sz[...] = jnp.transpose(gathered).reshape(NZ, 8, 128)

    with jax.named_scope("z_send"):
        each(1, NZ, lambda k: z_copy(sz, rz, zs_sem.at[0], zr_sem, nearness_to_offset(k)).start())
        rz[pl.ds(z, 1)] = sz[pl.ds(z, 1)]

    def evaluate(peer):
        weights = []
        for sl in range(4):
            lanes = slice(sl * 128, (sl + 1) * 128)
            w0 = jnp.broadcast_to(rz[peer, sl : sl + 1, :], (8, 128))
            w1 = jnp.broadcast_to(rz[peer, 4 + sl : 5 + sl, :], (8, 128))
            basis_r = lagrange(decode(lax.shift_right_logical(w0, 16)), consts)
            basis_s = lagrange(decode(jnp.bitwise_and(w0, 65535)), consts)
            basis_t = lagrange(decode(lax.shift_right_logical(w1, 16)), consts)
            element = jnp.bitwise_and(w1, 65535)
            weights.append(
                jnp.concatenate(
                    [jnp.where(element == e, basis_r, 0.0) for e in range(16)], axis=0
                ).astype(jnp.bfloat16)
            )
            for j in range(8):
                ts[j * 8 : (j + 1) * 8, lanes] = basis_s[j : j + 1, :] * basis_t
        for half in range(2):
            pair = jnp.concatenate(weights[2 * half : 2 * half + 2], axis=1)
            lanes = slice(half * 256, (half + 1) * 256)
            partial = jnp.dot(ft[...], pair, preferred_element_type=jnp.float32)
            total = None
            for n in range(64):
                term = partial[n * 16 : (n + 1) * 16, :] * ts[n : n + 1, lanes]
                total = term if total is None else total + term
            rounded = total.astype(jnp.bfloat16)
            vs[peer, 2 * half] = rounded[:, :128]
            vs[peer, 2 * half + 1] = rounded[:, 128:]

    with jax.named_scope("own"):
        evaluate(z)
        rv[pl.ds(z, 1)] = vs[pl.ds(z, 1)]

    def remote_step(k):
        offset = nearness_to_offset(position_to_nearness(k))
        with jax.named_scope("z_wait"):
            z_arrival(sz, rz, zs_sem.at[0], zr_sem, offset).wait_recv()
        with jax.named_scope("evaluate"):
            evaluate(lax.rem(z + offset, NZ))
            z_copy(vs, rv, vs_sem.at[0], vr_sem, offset).start()

    each(1, NZ, remote_step)

    def turn_back(n, at):
        offset = nearness_to_offset(position_to_nearness(n))
        block = rv[lax.rem(z + offset, NZ)].reshape(64, 128).astype(jnp.float32)
        rows = jnp.transpose(jnp.concatenate([block, pltpu.roll(block, 96, 1)], axis=0))
        for half in range(2):
            srf[pl.ds(2 * at + half, 32, stride=8), :] = rows[half * 64 : half * 64 + 32, :]

    def return_group(g, first):
        def wait(n):
            offset = nearness_to_offset(position_to_nearness(n))
            z_arrival(vs, rv, vs_sem.at[0], vr_sem, offset).wait_recv()

        with jax.named_scope("z_return"):
            each(first, 4 * g + 4, wait)
        with jax.named_scope("turn_back"):
            for at in range(4):
                turn_back(4 * g + at, at)
            sr[g] = srf[...].reshape(NQ, 8, 128).astype(jnp.bfloat16)
        with jax.named_scope("plane_return"):
            each(1, NQ, lambda k: plane_copy(sr.at[g], rr.at[g], ws_sem.at[g], wr_sem.at[g], k).start())
            pltpu.make_async_copy(sr.at[g, q], rr.at[g, q], own_sem.at[g]).start()

    for g in range(GROUPS):
        return_group(g, max(4 * g, 1))
    with jax.named_scope("drain"):
        plane_all(sq, rq, qs_sem.at[0], qr_sem.at[0]).wait_send()
        z_all(sz, rz, zs_sem.at[0], zr_sem).wait_send()
        z_all(vs, rv, vs_sem.at[0], vr_sem).wait_send()
    with jax.named_scope("plane_back"):
        for g in range(GROUPS):
            plane_all(sr.at[g], rr.at[g], ws_sem.at[g], wr_sem.at[g]).wait_recv()
            pltpu.make_async_copy(sr.at[g, q], rr.at[g, q], own_sem.at[g]).wait()
    with jax.named_scope("drain2"):
        for g in range(GROUPS):
            plane_all(sr.at[g], rr.at[g], ws_sem.at[g], wr_sem.at[g]).wait_send()


def finish(rr_hbm, out_hbm, rr, srf, orf, staged, sem, in_sem):
    loads = [pltpu.make_async_copy(rr_hbm.at[g], rr.at[g], in_sem.at[g]) for g in range(GROUPS)]
    for load in loads:
        load.start()
    z = lax.div(lax.axis_index("wide"), NY)

    with jax.named_scope("widen"):
        for g in range(GROUPS):
            loads[g].wait()
            srf[g] = rr[g].reshape(NQ * 8, 128).astype(jnp.float32)
    copies = []
    for t in range(4):
        with jax.named_scope("finish"):
            for half in range(2):
                parts = []
                for zl in range(4):
                    position = offset_to_position(lax.rem(t * 4 + zl - z + NZ, NZ))
                    row = lax.rem(position, 4) * 2 + half
                    parts.append(srf[lax.div(position, 4), pl.ds(row, 32, stride=8), :])
                turned = jnp.transpose(jnp.concatenate(parts, axis=0))
                for n in range(8):
                    orf[t, pl.ds(half * 8 + n, 16, stride=16), :] = turned[n * 16 : (n + 1) * 16, :]
            staged[t] = orf[t].reshape(16, 16, 128).astype(jnp.bfloat16)
            copy = pltpu.make_async_copy(
                staged.at[t], out_hbm.at[:, 0, :, pl.ds(t * 128, 128)], sem.at[t]
            )
            copy.start()
            copies.append(copy)
    with jax.named_scope("store"):
        for copy in copies:
            copy.wait()


def on_device(query_coords, owner_element, pair_counts, fields):
    anywhere = pl.BlockSpec(memory_space=pl.ANY)
    vmem = pl.BlockSpec(memory_space=pltpu.VMEM)
    returned = pl.pallas_call(
        kernel,
        out_shape=jax.ShapeDtypeStruct((GROUPS, NQ, 8, 128), jnp.bfloat16),
        in_specs=[anywhere] * 4,
        out_specs=anywhere,
        scratch_shapes=[
            pltpu.VMEM((3, 1, 16, 512), jnp.float32),
            pltpu.VMEM((1, 16, 512), jnp.int32),
            pltpu.VMEM((1, 512), jnp.int32),
            pltpu.VMEM((16, 8, 1024), jnp.bfloat16),
            pltpu.VMEM((1024, 128), jnp.bfloat16),
            pltpu.VMEM((1024, 128), jnp.float32),
            pltpu.VMEM((4, 8, 512), jnp.int32),
            pltpu.VMEM((NQ, 4, 128), jnp.int32),
            pltpu.VMEM((NQ, 4, 128), jnp.int32),
            pltpu.VMEM((NZ, 8, 128), jnp.int32),
            pltpu.VMEM((NZ, 8, 128), jnp.int32),
            pltpu.VMEM((64, 512), jnp.float32),
            pltpu.VMEM((NZ, 4, 16, 128), jnp.bfloat16),
            pltpu.VMEM((NZ, 4, 16, 128), jnp.bfloat16),
            pltpu.VMEM((NQ * 8, 128), jnp.float32),
            pltpu.VMEM((GROUPS, NQ, 8, 128), jnp.bfloat16),
            pltpu.SemaphoreType.DMA((4,)),
            pltpu.SemaphoreType.DMA((1,)),
            pltpu.SemaphoreType.DMA((1,)),
            pltpu.SemaphoreType.DMA((1,)),
            pltpu.SemaphoreType.DMA((NZ,)),
            pltpu.SemaphoreType.DMA((1,)),
            pltpu.SemaphoreType.DMA((NZ,)),
            pltpu.SemaphoreType.DMA((GROUPS,)),
            pltpu.SemaphoreType.DMA((GROUPS,)),
            pltpu.SemaphoreType.DMA((GROUPS,)),
            pltpu.SemaphoreType.REGULAR,
        ],
        compiler_params=pltpu.CompilerParams(collective_id=0, has_side_effects=True),
    )(query_coords, owner_element, pair_counts, fields)
    return pl.pallas_call(
        finish,
        out_shape=jax.ShapeDtypeStruct((16, 1, 16, 512), jnp.bfloat16),
        in_specs=[anywhere],
        out_specs=anywhere,
        scratch_shapes=[
            pltpu.VMEM((GROUPS, NQ, 8, 128), jnp.bfloat16),
            pltpu.VMEM((GROUPS, NQ * 8, 128), jnp.float32),
            pltpu.VMEM((4, 256, 128), jnp.float32),
            pltpu.VMEM((4, 16, 16, 128), jnp.bfloat16),
            pltpu.SemaphoreType.DMA((4,)),
            pltpu.SemaphoreType.DMA((GROUPS,)),
        ],
    )(returned)


def solution(mesh):
    placed = (
        P(None, ("wide", "narrow"), None, None),
        P(("wide", "narrow"), None, None),
        P(("wide", "narrow"), None),
        P(("wide", "narrow"), None, None),
    )
    return jax.shard_map(
        on_device,
        mesh=mesh,
        in_specs=placed,
        out_specs=P(None, ("wide", "narrow"), None, None),
        check_vma=False,
    )
```

```python
import functools

import jax
import jax.numpy as jnp
from jax import lax
from jax.experimental import pallas as pl
from jax.experimental.pallas import tpu as pltpu
from jax.sharding import PartitionSpec as P

GLL_NODES = (
    -1.0,
    -0.8717401485096066,
    -0.5917001814331423,
    -0.2092992179024789,
    0.2092992179024789,
    0.5917001814331423,
    0.8717401485096066,
    1.0,
)
LOGICAL = pl.DeviceIdType.LOGICAL
NZ = 16
NQ = 32
NY = 4
NX = 8
NEAR = 10
GROUPS = 4


def node_constants():
    rows = []
    scale = []
    for i in range(8):
        product = 1.0
        for m in range(8):
            if m != i:
                product *= GLL_NODES[i] - GLL_NODES[m]
        scale.append(1.0 / product)
    rows.append(scale)
    for k in range(1, 8):
        rows.append([GLL_NODES[(i + k) % 8] for i in range(8)])
    return rows


def sublane_constant(values):
    index = lax.broadcasted_iota(jnp.int32, (8, 128), 0)
    result = jnp.full((8, 128), values[0], jnp.float32)
    for i in range(1, 8):
        result = jnp.where(index == i, jnp.float32(values[i]), result)
    return result


def lagrange(position, consts):
    result = consts[0]
    for k in range(1, 8):
        result = result * (position - consts[k])
    return result


def encode(x):
    return (x * 32767.0 + 32768.5).astype(jnp.int32)


def decode(u):
    return (u - 32768).astype(jnp.float32) * jnp.float32(1.0 / 32767.0)


def position_to_nearness(k):
    late = lax.div(k + 15 - NEAR, 16)
    return k * (1 - late) + (NZ + NEAR - k) * late


def nearness_to_offset(n):
    return lax.rem(lax.div(n + 1, 2) * (1 - 2 * lax.rem(n, 2)) + NZ, NZ)


ORDER = (0, 15, 1, 14, 2, 13, 3, 12, 4, 11, 5, 8, 7, 9, 6, 10)


def each(low, high, do):
    def step(k, carry):
        do(k)
        return carry

    lax.fori_loop(low, high, step, 0)


def kernel(
    qc_hbm, oe_hbm, pc_hbm, fl_hbm, rr,
    qc, oe, pc, fl, ft, gf, ee, sq, rq, sz, rz, ts, vs, rv, srf, sr,
    in_sem, qs_sem, qr_sem, zs_sem, zr_sem, vs_sem, vr_sem, ws_sem, wr_sem, own_sem, told,
):
    wide = lax.axis_index("wide")
    narrow = lax.axis_index("narrow")
    z = lax.div(wide, NY)
    q = lax.rem(wide, NY) * NX + narrow
    me = z * NQ + q
    core = lax.rem(narrow, 2)

    def plane_peer(k):
        peer = lax.rem(q + k, NQ)
        return peer, z * NQ + peer

    def z_peer(o):
        peer = lax.rem(z + o, NZ)
        return peer, peer * NQ + q

    loads = [
        pltpu.make_async_copy(src, dst, in_sem.at[n])
        for n, (src, dst) in enumerate(((qc_hbm, qc), (oe_hbm, oe), (pc_hbm, pc), (fl_hbm, fl)))
    ]
    barrier = pltpu.get_barrier_semaphore()

    def greet_plane(k):
        chip = lax.rem(lax.div(q, 2) + k, NQ // 2)
        pl.semaphore_signal(barrier, inc=1, device_id=z * NQ + 2 * chip, device_id_type=LOGICAL)

    def greet_z(k):
        peer = z_peer(k)[1]
        pl.semaphore_signal(barrier, inc=1, device_id=peer - core + 1, device_id_type=LOGICAL)

    with jax.named_scope("greet"):
        for load in loads:
            load.start()
        for k in range(1, NQ // 2):
            greet_plane(k)

        @pl.when(core == 1)
        def _():
            pl.semaphore_signal(barrier, inc=1, device_id=me - 1, device_id_type=LOGICAL)

        for distance in range(NZ // 2, 0, -1):
            for offset in sorted({NZ - distance, distance}):
                greet_z(offset)

    with jax.named_scope("load"):
        for load in loads[:3]:
            load.wait()

    with jax.named_scope("encode"):
        for h in range(4):
            rows = pl.ds(4 * h, 4)
            slot = lax.broadcasted_iota(jnp.int32, (4, 512), 0) + 4 * h
            live = slot < pc[0:1, :]
            element = jnp.where(live, oe[0, rows, :], 16)
            ee[h, 0:4, :] = jnp.left_shift(encode(qc[0, 0, rows, :]), 16) + encode(qc[1, 0, rows, :])
            ee[h, 4:8, :] = jnp.left_shift(encode(qc[2, 0, rows, :]), 16) + element
        group = lax.broadcasted_iota(jnp.int32, (8, 128), 1) // 32
        blocks = []
        for t in range(4):
            pieces = [ee[h, :, t * 128 : (t + 1) * 128] for h in range(4)]
            for zl in range(4):
                block = None
                for h in range(4):
                    shift = ((h - zl) * 32) % 128
                    piece = pieces[h] if shift == 0 else pltpu.roll(pieces[h], shift, 1)
                    block = piece if block is None else jnp.where(group == h, piece, block)
                blocks.append(block)
        turned = jnp.transpose(jnp.concatenate(blocks, axis=0))
        for h in range(4):
            sq[:, h, :] = turned[h * 32 : (h + 1) * 32, :]

    with jax.named_scope("barrier"):

        @pl.when(core == 0)
        def _():
            pl.semaphore_wait(barrier, NQ - 1)
            pl.semaphore_signal(told, inc=1, device_id=me + 1, device_id_type=LOGICAL)

        @pl.when(core == 1)
        def _():
            pl.semaphore_wait(told, 1)

    def plane_copy(src, dst, send, recv, k):
        peer, device = plane_peer(k)
        return pltpu.make_async_remote_copy(
            src_ref=src.at[peer], dst_ref=dst.at[q], send_sem=send, recv_sem=recv,
            device_id=device, device_id_type=LOGICAL,
        )

    def plane_all(src, dst, send, recv):
        others = pl.ds(0, NQ - 1)
        return pltpu.make_async_remote_copy(
            src_ref=src.at[others], dst_ref=dst.at[others], send_sem=send, recv_sem=recv,
            device_id=plane_peer(1)[1], device_id_type=LOGICAL,
        )

    def z_copy(src, dst, send, recv, o):
        peer, device = z_peer(o)
        return pltpu.make_async_remote_copy(
            src_ref=src.at[peer], dst_ref=dst.at[z], send_sem=send, recv_sem=recv.at[z],
            device_id=device, device_id_type=LOGICAL,
        )

    def z_arrival(src, dst, send, recv, o):
        peer, device = z_peer(o)
        return pltpu.make_async_remote_copy(
            src_ref=src.at[peer], dst_ref=dst.at[peer], send_sem=send, recv_sem=recv.at[peer],
            device_id=device, device_id_type=LOGICAL,
        )

    def z_all(src, dst, send, recv):
        others = pl.ds(0, NZ - 1)
        return pltpu.make_async_remote_copy(
            src_ref=src.at[others], dst_ref=dst.at[others], send_sem=send, recv_sem=recv.at[0],
            device_id=z_peer(1)[1], device_id_type=LOGICAL,
        )

    with jax.named_scope("plane_send"):
        for k in range(1, NQ):
            plane_copy(sq, rq, qs_sem.at[0], qr_sem.at[0], k).start()
        rq[pl.ds(q, 1)] = sq[pl.ds(q, 1)]

    def permute(n):
        ft[pl.ds(pl.multiple_of(n * 16, 16), 16), :] = gf[pl.ds(n, 16, stride=64), :].astype(jnp.bfloat16)

    with jax.named_scope("table"):
        loads[3].wait()
        for b in range(8):
            part = fl[:, :, b * 128 : (b + 1) * 128].reshape(128, 128).astype(jnp.float32)
            gf[b * 128 : (b + 1) * 128, :] = jnp.transpose(part)
        each(0, 64, permute)
    consts = [sublane_constant(v) for v in node_constants()]

    with jax.named_scope("barrier_z"):

        @pl.when(core == 1)
        def _():
            pl.semaphore_wait(barrier, 2 * (NZ - 1))
            pl.semaphore_signal(told, inc=1, device_id=me - 1, device_id_type=LOGICAL)

        @pl.when(core == 0)
        def _():
            pl.semaphore_wait(told, 1)

    with jax.named_scope("plane_wait"):
        plane_all(sq, rq, qs_sem.at[0], qr_sem.at[0]).wait_recv()
    with jax.named_scope("turn_queries"):
        gathered = jnp.concatenate([rq[:, h, :] for h in range(4)], axis=0)
        sz[...] = jnp.transpose(gathered).reshape(NZ, 8, 128)

    with jax.named_scope("z_send"):
        for distance in range(1, NZ // 2 + 1):
            for offset in sorted({NZ - distance, distance}, reverse=True):
                z_copy(sz, rz, zs_sem.at[0], zr_sem, offset).start()
        rz[pl.ds(z, 1)] = sz[pl.ds(z, 1)]

    def evaluate(peer):
        weights = []
        for sl in range(4):
            lanes = slice(sl * 128, (sl + 1) * 128)
            w0 = jnp.broadcast_to(rz[peer, sl : sl + 1, :], (8, 128))
            w1 = jnp.broadcast_to(rz[peer, 4 + sl : 5 + sl, :], (8, 128))
            basis_r = lagrange(decode(lax.shift_right_logical(w0, 16)), consts)
            basis_s = lagrange(decode(jnp.bitwise_and(w0, 65535)), consts)
            basis_t = lagrange(decode(lax.shift_right_logical(w1, 16)), consts)
            element = jnp.bitwise_and(w1, 65535)
            weights.append(
                jnp.concatenate(
                    [jnp.where(element == e, basis_r, 0.0) for e in range(16)], axis=0
                ).astype(jnp.bfloat16)
            )
            for j in range(8):
                ts[j * 8 : (j + 1) * 8, lanes] = basis_s[j : j + 1, :] * basis_t
        for half in range(2):
            pair = jnp.concatenate(weights[2 * half : 2 * half + 2], axis=1)
            lanes = slice(half * 256, (half + 1) * 256)
            partial = jnp.dot(ft[...], pair, preferred_element_type=jnp.float32)
            total = None
            for n in range(64):
                term = partial[n * 16 : (n + 1) * 16, :] * ts[n : n + 1, lanes]
                total = term if total is None else total + term
            rounded = total.astype(jnp.bfloat16)
            vs[peer, 2 * half] = rounded[:, :128]
            vs[peer, 2 * half + 1] = rounded[:, 128:]

    with jax.named_scope("own"):
        evaluate(z)
        rv[pl.ds(z, 1)] = vs[pl.ds(z, 1)]

    def remote_step(k):
        offset = nearness_to_offset(position_to_nearness(k))
        with jax.named_scope("z_wait"):
            z_arrival(sz, rz, zs_sem.at[0], zr_sem, offset).wait_recv()
        with jax.named_scope("evaluate"):
            evaluate(lax.rem(z + offset, NZ))
            z_copy(vs, rv, vs_sem.at[0], vr_sem, offset).start()

    each(1, NZ, remote_step)

    def turn_back(n, at):
        block = rv[lax.rem(z + ORDER[n], NZ)].reshape(64, 128).astype(jnp.float32)
        rows = jnp.transpose(jnp.concatenate([block, pltpu.roll(block, 96, 1)], axis=0))
        for half in range(2):
            srf[pl.ds(2 * at + half, 32, stride=8), :] = rows[half * 64 : half * 64 + 32, :]

    def return_group(g, first):
        with jax.named_scope("z_return"):
            for n in range(first, 4 * g + 4):
                z_arrival(vs, rv, vs_sem.at[0], vr_sem, ORDER[n]).wait_recv()
        with jax.named_scope("turn_back"):
            for at in range(4):
                turn_back(4 * g + at, at)
            sr[g] = srf[...].reshape(NQ, 8, 128).astype(jnp.bfloat16)
        with jax.named_scope("plane_return"):
            for k in range(1, NQ):
                plane_copy(sr.at[g], rr.at[g], ws_sem.at[g], wr_sem.at[g], k).start()
            pltpu.make_async_copy(sr.at[g, q], rr.at[g, q], own_sem.at[g]).start()

    for g in range(GROUPS):
        return_group(g, max(4 * g, 1))
    with jax.named_scope("drain"):
        plane_all(sq, rq, qs_sem.at[0], qr_sem.at[0]).wait_send()
        z_all(sz, rz, zs_sem.at[0], zr_sem).wait_send()
        z_all(vs, rv, vs_sem.at[0], vr_sem).wait_send()
    with jax.named_scope("plane_back"):
        for g in range(GROUPS):
            plane_all(sr.at[g], rr.at[g], ws_sem.at[g], wr_sem.at[g]).wait_recv()
            pltpu.make_async_copy(sr.at[g, q], rr.at[g, q], own_sem.at[g]).wait()
    with jax.named_scope("drain2"):
        for g in range(GROUPS):
            plane_all(sr.at[g], rr.at[g], ws_sem.at[g], wr_sem.at[g]).wait_send()


def finish(rr_hbm, out_hbm, rr, srf, rows, orf, staged, sem, in_sem):
    loads = [pltpu.make_async_copy(rr_hbm.at[g], rr.at[g], in_sem.at[g]) for g in range(GROUPS)]
    for load in loads:
        load.start()
    z = lax.div(lax.axis_index("wide"), NY)

    with jax.named_scope("widen"):
        for g in range(GROUPS):
            loads[g].wait()
            srf[g] = rr[g].reshape(NQ * 8, 128).astype(jnp.float32)
            for n in range(4):
                owner = lax.rem(z + ORDER[4 * g + n], NZ)
                for half in range(2):
                    rows[owner, half] = srf[g, pl.ds(2 * n + half, NQ, stride=8), :]
    copies = []
    for t in range(4):
        with jax.named_scope("finish"):
            for half in range(2):
                turned = jnp.transpose(jnp.concatenate([rows[t * 4 + zl, half] for zl in range(4)], axis=0))
                for n in range(8):
                    orf[t, pl.ds(half * 8 + n, 16, stride=16), :] = turned[n * 16 : (n + 1) * 16, :]
            staged[t] = orf[t].reshape(16, 16, 128).astype(jnp.bfloat16)
            copy = pltpu.make_async_copy(
                staged.at[t], out_hbm.at[:, 0, :, pl.ds(t * 128, 128)], sem.at[t]
            )
            copy.start()
            copies.append(copy)
    with jax.named_scope("store"):
        for copy in copies:
            copy.wait()


def on_device(query_coords, owner_element, pair_counts, fields):
    anywhere = pl.BlockSpec(memory_space=pl.ANY)
    vmem = pl.BlockSpec(memory_space=pltpu.VMEM)
    returned = pl.pallas_call(
        kernel,
        out_shape=jax.ShapeDtypeStruct((GROUPS, NQ, 8, 128), jnp.bfloat16),
        in_specs=[anywhere] * 4,
        out_specs=anywhere,
        scratch_shapes=[
            pltpu.VMEM((3, 1, 16, 512), jnp.float32),
            pltpu.VMEM((1, 16, 512), jnp.int32),
            pltpu.VMEM((1, 512), jnp.int32),
            pltpu.VMEM((16, 8, 1024), jnp.bfloat16),
            pltpu.VMEM((1024, 128), jnp.bfloat16),
            pltpu.VMEM((1024, 128), jnp.float32),
            pltpu.VMEM((4, 8, 512), jnp.int32),
            pltpu.VMEM((NQ, 4, 128), jnp.int32),
            pltpu.VMEM((NQ, 4, 128), jnp.int32),
            pltpu.VMEM((NZ, 8, 128), jnp.int32),
            pltpu.VMEM((NZ, 8, 128), jnp.int32),
            pltpu.VMEM((64, 512), jnp.float32),
            pltpu.VMEM((NZ, 4, 16, 128), jnp.bfloat16),
            pltpu.VMEM((NZ, 4, 16, 128), jnp.bfloat16),
            pltpu.VMEM((NQ * 8, 128), jnp.float32),
            pltpu.VMEM((GROUPS, NQ, 8, 128), jnp.bfloat16),
            pltpu.SemaphoreType.DMA((4,)),
            pltpu.SemaphoreType.DMA((1,)),
            pltpu.SemaphoreType.DMA((1,)),
            pltpu.SemaphoreType.DMA((1,)),
            pltpu.SemaphoreType.DMA((NZ,)),
            pltpu.SemaphoreType.DMA((1,)),
            pltpu.SemaphoreType.DMA((NZ,)),
            pltpu.SemaphoreType.DMA((GROUPS,)),
            pltpu.SemaphoreType.DMA((GROUPS,)),
            pltpu.SemaphoreType.DMA((GROUPS,)),
            pltpu.SemaphoreType.REGULAR,
        ],
        compiler_params=pltpu.CompilerParams(collective_id=0, has_side_effects=True),
    )(query_coords, owner_element, pair_counts, fields)
    return pl.pallas_call(
        finish,
        out_shape=jax.ShapeDtypeStruct((16, 1, 16, 512), jnp.bfloat16),
        in_specs=[anywhere],
        out_specs=anywhere,
        scratch_shapes=[
            pltpu.VMEM((GROUPS, NQ, 8, 128), jnp.bfloat16),
            pltpu.VMEM((GROUPS, NQ * 8, 128), jnp.float32),
            pltpu.VMEM((NZ, 2, NQ, 128), jnp.float32),
            pltpu.VMEM((4, 256, 128), jnp.float32),
            pltpu.VMEM((4, 16, 16, 128), jnp.bfloat16),
            pltpu.SemaphoreType.DMA((4,)),
            pltpu.SemaphoreType.DMA((GROUPS,)),
        ],
    )(returned)


def solution(mesh):
    placed = (
        P(None, ("wide", "narrow"), None, None),
        P(("wide", "narrow"), None, None),
        P(("wide", "narrow"), None),
        P(("wide", "narrow"), None, None),
    )
    return jax.shard_map(
        on_device,
        mesh=mesh,
        in_specs=placed,
        out_specs=P(None, ("wide", "narrow"), None, None),
        check_vma=False,
    )
```

```python
import functools

import jax
import jax.numpy as jnp
from jax import lax
from jax.experimental import pallas as pl
from jax.experimental.pallas import tpu as pltpu
from jax.sharding import PartitionSpec as P

GLL_NODES = (
    -1.0,
    -0.8717401485096066,
    -0.5917001814331423,
    -0.2092992179024789,
    0.2092992179024789,
    0.5917001814331423,
    0.8717401485096066,
    1.0,
)
LOGICAL = pl.DeviceIdType.LOGICAL
NZ = 16
NQ = 32
NY = 4
NX = 8
NEAR = 10
GROUPS = 4


def node_constants():
    rows = []
    scale = []
    for i in range(8):
        product = 1.0
        for m in range(8):
            if m != i:
                product *= GLL_NODES[i] - GLL_NODES[m]
        scale.append(1.0 / product)
    rows.append(scale)
    for k in range(1, 8):
        rows.append([GLL_NODES[(i + k) % 8] for i in range(8)])
    return rows


def sublane_constant(values):
    index = lax.broadcasted_iota(jnp.int32, (8, 128), 0)
    result = jnp.full((8, 128), values[0], jnp.float32)
    for i in range(1, 8):
        result = jnp.where(index == i, jnp.float32(values[i]), result)
    return result


def lagrange(position, consts):
    result = consts[0]
    for k in range(1, 8):
        result = result * (position - consts[k])
    return result


def encode(x):
    return (x * 32767.0 + 32768.5).astype(jnp.int32)


def decode(u):
    return (u - 32768).astype(jnp.float32) * jnp.float32(1.0 / 32767.0)


def position_to_nearness(k, near):
    late = lax.div(k + 15 - near, 16)
    return k * (1 - late) + (NZ + near - k) * late


def nearness_to_offset(n):
    return lax.rem(lax.div(n + 1, 2) * (1 - 2 * lax.rem(n, 2)) + NZ, NZ)


ORDER = (0, 15, 1, 14, 2, 13, 3, 12, 4, 11, 5, 8, 7, 9, 6, 10)


def each(low, high, do):
    def step(k, carry):
        do(k)
        return carry

    lax.fori_loop(low, high, step, 0)


def kernel(
    qc_hbm, oe_hbm, pc_hbm, fl_hbm, rr,
    qc, oe, pc, fl, ft, gf, ee, sq, rq, sz, rz, ts, vs, rv, srf, sr,
    in_sem, qs_sem, qr_sem, zs_sem, zr_sem, vs_sem, vr_sem, ws_sem, wr_sem, own_sem, told,
):
    wide = lax.axis_index("wide")
    narrow = lax.axis_index("narrow")
    z = lax.div(wide, NY)
    q = lax.rem(wide, NY) * NX + narrow
    me = z * NQ + q
    core = lax.rem(narrow, 2)

    def plane_peer(k):
        peer = lax.rem(q + k, NQ)
        return peer, z * NQ + peer

    def z_peer(o):
        peer = lax.rem(z + o, NZ)
        return peer, peer * NQ + q

    loads = [
        pltpu.make_async_copy(src, dst, in_sem.at[n])
        for n, (src, dst) in enumerate(((qc_hbm, qc), (oe_hbm, oe), (pc_hbm, pc), (fl_hbm, fl)))
    ]
    barrier = pltpu.get_barrier_semaphore()

    def greet_plane(k):
        chip = lax.rem(lax.div(q, 2) + k, NQ // 2)
        pl.semaphore_signal(barrier, inc=1, device_id=z * NQ + 2 * chip, device_id_type=LOGICAL)

    def greet_z(k):
        peer = z_peer(k)[1]
        pl.semaphore_signal(barrier, inc=1, device_id=peer - core + 1, device_id_type=LOGICAL)

    with jax.named_scope("greet"):
        for load in loads:
            load.start()
        for k in range(1, NQ // 2):
            greet_plane(k)

        @pl.when(core == 1)
        def _():
            pl.semaphore_signal(barrier, inc=1, device_id=me - 1, device_id_type=LOGICAL)

        for distance in range(NZ // 2, 0, -1):
            for offset in sorted({NZ - distance, distance}):
                greet_z(offset)

    with jax.named_scope("load"):
        for load in loads[:3]:
            load.wait()

    with jax.named_scope("encode"):
        for h in range(4):
            rows = pl.ds(4 * h, 4)
            slot = lax.broadcasted_iota(jnp.int32, (4, 512), 0) + 4 * h
            live = slot < pc[0:1, :]
            element = jnp.where(live, oe[0, rows, :], 16)
            ee[h, 0:4, :] = jnp.left_shift(encode(qc[0, 0, rows, :]), 16) + encode(qc[1, 0, rows, :])
            ee[h, 4:8, :] = jnp.left_shift(encode(qc[2, 0, rows, :]), 16) + element
        group = lax.broadcasted_iota(jnp.int32, (8, 128), 1) // 32
        blocks = []
        for t in range(4):
            pieces = [ee[h, :, t * 128 : (t + 1) * 128] for h in range(4)]
            for zl in range(4):
                block = None
                for h in range(4):
                    shift = ((h - zl) * 32) % 128
                    piece = pieces[h] if shift == 0 else pltpu.roll(pieces[h], shift, 1)
                    block = piece if block is None else jnp.where(group == h, piece, block)
                blocks.append(block)
        turned = jnp.transpose(jnp.concatenate(blocks, axis=0))
        for h in range(4):
            sq[:, h, :] = turned[h * 32 : (h + 1) * 32, :]

    with jax.named_scope("barrier"):

        @pl.when(core == 0)
        def _():
            pl.semaphore_wait(barrier, NQ - 1)
            pl.semaphore_signal(told, inc=1, device_id=me + 1, device_id_type=LOGICAL)

        @pl.when(core == 1)
        def _():
            pl.semaphore_wait(told, 1)

    def plane_copy(src, dst, send, recv, k):
        peer, device = plane_peer(k)
        return pltpu.make_async_remote_copy(
            src_ref=src.at[peer], dst_ref=dst.at[q], send_sem=send, recv_sem=recv,
            device_id=device, device_id_type=LOGICAL,
        )

    def plane_all(src, dst, send, recv):
        others = pl.ds(0, NQ - 1)
        return pltpu.make_async_remote_copy(
            src_ref=src.at[others], dst_ref=dst.at[others], send_sem=send, recv_sem=recv,
            device_id=plane_peer(1)[1], device_id_type=LOGICAL,
        )

    def z_copy(src, dst, send, recv, o):
        peer, device = z_peer(o)
        return pltpu.make_async_remote_copy(
            src_ref=src.at[peer], dst_ref=dst.at[z], send_sem=send, recv_sem=recv.at[z],
            device_id=device, device_id_type=LOGICAL,
        )

    def z_arrival(src, dst, send, recv, o):
        peer, device = z_peer(o)
        return pltpu.make_async_remote_copy(
            src_ref=src.at[peer], dst_ref=dst.at[peer], send_sem=send, recv_sem=recv.at[peer],
            device_id=device, device_id_type=LOGICAL,
        )

    def z_all(src, dst, send, recv):
        others = pl.ds(0, NZ - 1)
        return pltpu.make_async_remote_copy(
            src_ref=src.at[others], dst_ref=dst.at[others], send_sem=send, recv_sem=recv.at[0],
            device_id=z_peer(1)[1], device_id_type=LOGICAL,
        )

    with jax.named_scope("plane_send"):
        for k in range(1, NQ):
            plane_copy(sq, rq, qs_sem.at[0], qr_sem.at[0], k).start()
        rq[pl.ds(q, 1)] = sq[pl.ds(q, 1)]

    def permute(n):
        ft[pl.ds(pl.multiple_of(n * 16, 16), 16), :] = gf[pl.ds(n, 16, stride=64), :].astype(jnp.bfloat16)

    with jax.named_scope("table"):
        loads[3].wait()
        for b in range(8):
            part = fl[:, :, b * 128 : (b + 1) * 128].reshape(128, 128).astype(jnp.float32)
            gf[b * 128 : (b + 1) * 128, :] = jnp.transpose(part)
        each(0, 64, permute)
    consts = [sublane_constant(v) for v in node_constants()]

    with jax.named_scope("barrier_z"):

        @pl.when(core == 1)
        def _():
            pl.semaphore_wait(barrier, 2 * (NZ - 1))
            pl.semaphore_signal(told, inc=1, device_id=me - 1, device_id_type=LOGICAL)

        @pl.when(core == 0)
        def _():
            pl.semaphore_wait(told, 1)

    with jax.named_scope("plane_wait"):
        plane_all(sq, rq, qs_sem.at[0], qr_sem.at[0]).wait_recv()
    with jax.named_scope("turn_queries"):
        gathered = jnp.concatenate([rq[:, h, :] for h in range(4)], axis=0)
        sz[...] = jnp.transpose(gathered).reshape(NZ, 8, 128)

    with jax.named_scope("z_send"):
        for distance in range(1, NZ // 2 + 1):
            for offset in sorted({NZ - distance, distance}, reverse=True):
                z_copy(sz, rz, zs_sem.at[0], zr_sem, offset).start()
        rz[pl.ds(z, 1)] = sz[pl.ds(z, 1)]

    def evaluate(peer):
        weights = []
        for sl in range(4):
            lanes = slice(sl * 128, (sl + 1) * 128)
            w0 = jnp.broadcast_to(rz[peer, sl : sl + 1, :], (8, 128))
            w1 = jnp.broadcast_to(rz[peer, 4 + sl : 5 + sl, :], (8, 128))
            basis_r = lagrange(decode(lax.shift_right_logical(w0, 16)), consts)
            basis_s = lagrange(decode(jnp.bitwise_and(w0, 65535)), consts)
            basis_t = lagrange(decode(lax.shift_right_logical(w1, 16)), consts)
            element = jnp.bitwise_and(w1, 65535)
            weights.append(
                jnp.concatenate(
                    [jnp.where(element == e, basis_r, 0.0) for e in range(16)], axis=0
                ).astype(jnp.bfloat16)
            )
            for j in range(8):
                ts[j * 8 : (j + 1) * 8, lanes] = basis_s[j : j + 1, :] * basis_t
        for half in range(2):
            pair = jnp.concatenate(weights[2 * half : 2 * half + 2], axis=1)
            lanes = slice(half * 256, (half + 1) * 256)
            partial = jnp.dot(ft[...], pair, preferred_element_type=jnp.float32)
            total = None
            for n in range(64):
                term = partial[n * 16 : (n + 1) * 16, :] * ts[n : n + 1, lanes]
                total = term if total is None else total + term
            rounded = total.astype(jnp.bfloat16)
            vs[peer, 2 * half] = rounded[:, :128]
            vs[peer, 2 * half + 1] = rounded[:, 128:]

    with jax.named_scope("own"):
        evaluate(z)
        rv[pl.ds(z, 1)] = vs[pl.ds(z, 1)]

    def remote_step(k):
        offset = nearness_to_offset(position_to_nearness(k, 10 - 4 * core))
        with jax.named_scope("z_wait"):
            z_arrival(sz, rz, zs_sem.at[0], zr_sem, offset).wait_recv()
        with jax.named_scope("evaluate"):
            evaluate(lax.rem(z + offset, NZ))
            z_copy(vs, rv, vs_sem.at[0], vr_sem, offset).start()

    each(1, NZ, remote_step)

    def turn_back(n, at):
        block = rv[lax.rem(z + ORDER[n], NZ)].reshape(64, 128).astype(jnp.float32)
        rows = jnp.transpose(jnp.concatenate([block, pltpu.roll(block, 96, 1)], axis=0))
        for half in range(2):
            srf[pl.ds(2 * at + half, 32, stride=8), :] = rows[half * 64 : half * 64 + 32, :]

    def return_group(g, first):
        with jax.named_scope("z_return"):
            for n in range(first, 4 * g + 4):
                z_arrival(vs, rv, vs_sem.at[0], vr_sem, ORDER[n]).wait_recv()
        with jax.named_scope("turn_back"):
            for at in range(4):
                turn_back(4 * g + at, at)
            sr[g] = srf[...].reshape(NQ, 8, 128).astype(jnp.bfloat16)
        with jax.named_scope("plane_return"):
            for k in range(1, NQ):
                plane_copy(sr.at[g], rr.at[g], ws_sem.at[g], wr_sem.at[g], k).start()
            pltpu.make_async_copy(sr.at[g, q], rr.at[g, q], own_sem.at[g]).start()

    for g in range(GROUPS):
        return_group(g, max(4 * g, 1))
    with jax.named_scope("drain"):
        plane_all(sq, rq, qs_sem.at[0], qr_sem.at[0]).wait_send()
        z_all(sz, rz, zs_sem.at[0], zr_sem).wait_send()
        z_all(vs, rv, vs_sem.at[0], vr_sem).wait_send()
    with jax.named_scope("plane_back"):
        for g in range(GROUPS):
            plane_all(sr.at[g], rr.at[g], ws_sem.at[g], wr_sem.at[g]).wait_recv()
            pltpu.make_async_copy(sr.at[g, q], rr.at[g, q], own_sem.at[g]).wait()
    with jax.named_scope("drain2"):
        for g in range(GROUPS):
            plane_all(sr.at[g], rr.at[g], ws_sem.at[g], wr_sem.at[g]).wait_send()


def finish(rr_hbm, out_hbm, rr, srf, rows, orf, staged, sem, in_sem):
    loads = [pltpu.make_async_copy(rr_hbm.at[g], rr.at[g], in_sem.at[g]) for g in range(GROUPS)]
    for load in loads:
        load.start()
    z = lax.div(lax.axis_index("wide"), NY)

    with jax.named_scope("widen"):
        for g in range(GROUPS):
            loads[g].wait()
            srf[g] = rr[g].reshape(NQ * 8, 128).astype(jnp.float32)
            for n in range(4):
                owner = lax.rem(z + ORDER[4 * g + n], NZ)
                for half in range(2):
                    rows[owner, half] = srf[g, pl.ds(2 * n + half, NQ, stride=8), :]
    copies = []
    for t in range(4):
        with jax.named_scope("finish"):
            for half in range(2):
                turned = jnp.transpose(jnp.concatenate([rows[t * 4 + zl, half] for zl in range(4)], axis=0))
                for n in range(8):
                    orf[t, pl.ds(half * 8 + n, 16, stride=16), :] = turned[n * 16 : (n + 1) * 16, :]
            staged[t] = orf[t].reshape(16, 16, 128).astype(jnp.bfloat16)
            copy = pltpu.make_async_copy(
                staged.at[t], out_hbm.at[:, 0, :, pl.ds(t * 128, 128)], sem.at[t]
            )
            copy.start()
            copies.append(copy)
    with jax.named_scope("store"):
        for copy in copies:
            copy.wait()


def on_device(query_coords, owner_element, pair_counts, fields):
    anywhere = pl.BlockSpec(memory_space=pl.ANY)
    vmem = pl.BlockSpec(memory_space=pltpu.VMEM)
    returned = pl.pallas_call(
        kernel,
        out_shape=jax.ShapeDtypeStruct((GROUPS, NQ, 8, 128), jnp.bfloat16),
        in_specs=[anywhere] * 4,
        out_specs=anywhere,
        scratch_shapes=[
            pltpu.VMEM((3, 1, 16, 512), jnp.float32),
            pltpu.VMEM((1, 16, 512), jnp.int32),
            pltpu.VMEM((1, 512), jnp.int32),
            pltpu.VMEM((16, 8, 1024), jnp.bfloat16),
            pltpu.VMEM((1024, 128), jnp.bfloat16),
            pltpu.VMEM((1024, 128), jnp.float32),
            pltpu.VMEM((4, 8, 512), jnp.int32),
            pltpu.VMEM((NQ, 4, 128), jnp.int32),
            pltpu.VMEM((NQ, 4, 128), jnp.int32),
            pltpu.VMEM((NZ, 8, 128), jnp.int32),
            pltpu.VMEM((NZ, 8, 128), jnp.int32),
            pltpu.VMEM((64, 512), jnp.float32),
            pltpu.VMEM((NZ, 4, 16, 128), jnp.bfloat16),
            pltpu.VMEM((NZ, 4, 16, 128), jnp.bfloat16),
            pltpu.VMEM((NQ * 8, 128), jnp.float32),
            pltpu.VMEM((GROUPS, NQ, 8, 128), jnp.bfloat16),
            pltpu.SemaphoreType.DMA((4,)),
            pltpu.SemaphoreType.DMA((1,)),
            pltpu.SemaphoreType.DMA((1,)),
            pltpu.SemaphoreType.DMA((1,)),
            pltpu.SemaphoreType.DMA((NZ,)),
            pltpu.SemaphoreType.DMA((1,)),
            pltpu.SemaphoreType.DMA((NZ,)),
            pltpu.SemaphoreType.DMA((GROUPS,)),
            pltpu.SemaphoreType.DMA((GROUPS,)),
            pltpu.SemaphoreType.DMA((GROUPS,)),
            pltpu.SemaphoreType.REGULAR,
        ],
        compiler_params=pltpu.CompilerParams(collective_id=0, has_side_effects=True),
    )(query_coords, owner_element, pair_counts, fields)
    return pl.pallas_call(
        finish,
        out_shape=jax.ShapeDtypeStruct((16, 1, 16, 512), jnp.bfloat16),
        in_specs=[anywhere],
        out_specs=anywhere,
        scratch_shapes=[
            pltpu.VMEM((GROUPS, NQ, 8, 128), jnp.bfloat16),
            pltpu.VMEM((GROUPS, NQ * 8, 128), jnp.float32),
            pltpu.VMEM((NZ, 2, NQ, 128), jnp.float32),
            pltpu.VMEM((4, 256, 128), jnp.float32),
            pltpu.VMEM((4, 16, 16, 128), jnp.bfloat16),
            pltpu.SemaphoreType.DMA((4,)),
            pltpu.SemaphoreType.DMA((GROUPS,)),
        ],
    )(returned)


def solution(mesh):
    placed = (
        P(None, ("wide", "narrow"), None, None),
        P(("wide", "narrow"), None, None),
        P(("wide", "narrow"), None),
        P(("wide", "narrow"), None, None),
    )
    return jax.shard_map(
        on_device,
        mesh=mesh,
        in_specs=placed,
        out_specs=P(None, ("wide", "narrow"), None, None),
        check_vma=False,
    )
```

```python
import functools

import jax
import jax.numpy as jnp
from jax import lax
from jax.experimental import pallas as pl
from jax.experimental.pallas import tpu as pltpu
from jax.sharding import PartitionSpec as P

GLL_NODES = (
    -1.0,
    -0.8717401485096066,
    -0.5917001814331423,
    -0.2092992179024789,
    0.2092992179024789,
    0.5917001814331423,
    0.8717401485096066,
    1.0,
)
LOGICAL = pl.DeviceIdType.LOGICAL
NZ = 16
NQ = 32
NY = 4
NX = 8
NEAR = 10
GROUPS = 4


def node_constants():
    rows = []
    scale = []
    for i in range(8):
        product = 1.0
        for m in range(8):
            if m != i:
                product *= GLL_NODES[i] - GLL_NODES[m]
        scale.append(1.0 / product)
    rows.append(scale)
    for k in range(1, 8):
        rows.append([GLL_NODES[(i + k) % 8] for i in range(8)])
    return rows


def sublane_constant(values):
    index = lax.broadcasted_iota(jnp.int32, (8, 128), 0)
    result = jnp.full((8, 128), values[0], jnp.float32)
    for i in range(1, 8):
        result = jnp.where(index == i, jnp.float32(values[i]), result)
    return result


def lagrange(position, consts):
    result = consts[0]
    for k in range(1, 8):
        result = result * (position - consts[k])
    return result


def encode(x):
    return (x * 32767.0 + 32768.5).astype(jnp.int32)


def decode(u):
    return (u - 32768).astype(jnp.float32) * jnp.float32(1.0 / 32767.0)


def position_to_nearness(k, near):
    late = lax.div(k + 15 - near, 16)
    return k * (1 - late) + (NZ + near - k) * late


def nearness_to_offset(n):
    return lax.rem(lax.div(n + 1, 2) * (1 - 2 * lax.rem(n, 2)) + NZ, NZ)


ORDER = (0, 15, 1, 14, 2, 13, 3, 12, 4, 11, 5, 8, 7, 9, 6, 10)


def each(low, high, do):
    def step(k, carry):
        do(k)
        return carry

    lax.fori_loop(low, high, step, 0)


def kernel(
    qc_hbm, oe_hbm, pc_hbm, fl_hbm, rr,
    qc, oe, pc, fl, ft, gf, ee, sq, rq, sz, rz, ts, vs, rv, srf, sr,
    in_sem, qs_sem, qr_sem, zs_sem, zr_sem, vs_sem, vr_sem, ws_sem, wr_sem, own_sem, told,
):
    wide = lax.axis_index("wide")
    narrow = lax.axis_index("narrow")
    z = lax.div(wide, NY)
    q = lax.rem(wide, NY) * NX + narrow
    me = z * NQ + q
    core = lax.rem(narrow, 2)

    def plane_peer(k):
        peer = lax.rem(q + k, NQ)
        return peer, z * NQ + peer

    def z_peer(o):
        peer = lax.rem(z + o, NZ)
        return peer, peer * NQ + q

    loads = [
        pltpu.make_async_copy(src, dst, in_sem.at[n])
        for n, (src, dst) in enumerate(((qc_hbm, qc), (oe_hbm, oe), (pc_hbm, pc), (fl_hbm, fl)))
    ]
    barrier = pltpu.get_barrier_semaphore()

    def greet_plane(k):
        chip = lax.rem(lax.div(q, 2) + k, NQ // 2)
        pl.semaphore_signal(barrier, inc=1, device_id=z * NQ + 2 * chip, device_id_type=LOGICAL)

    def greet_z(k):
        peer = z_peer(k)[1]
        pl.semaphore_signal(barrier, inc=1, device_id=peer - core + 1, device_id_type=LOGICAL)

    with jax.named_scope("greet"):
        for load in loads:
            load.start()
        for k in range(1, NQ // 2):
            greet_plane(k)

        @pl.when(core == 1)
        def _():
            pl.semaphore_signal(barrier, inc=1, device_id=me - 1, device_id_type=LOGICAL)

        for distance in range(NZ // 2, 0, -1):
            for offset in sorted({NZ - distance, distance}):
                greet_z(offset)

    with jax.named_scope("load"):
        for load in loads[:3]:
            load.wait()

    with jax.named_scope("encode"):
        for h in range(4):
            rows = pl.ds(4 * h, 4)
            slot = lax.broadcasted_iota(jnp.int32, (4, 512), 0) + 4 * h
            live = slot < pc[0:1, :]
            element = jnp.where(live, oe[0, rows, :], 16)
            ee[h, 0:4, :] = jnp.left_shift(encode(qc[0, 0, rows, :]), 16) + encode(qc[1, 0, rows, :])
            ee[h, 4:8, :] = jnp.left_shift(encode(qc[2, 0, rows, :]), 16) + element
        group = lax.broadcasted_iota(jnp.int32, (8, 128), 1) // 32
        blocks = []
        for t in range(4):
            pieces = [ee[h, :, t * 128 : (t + 1) * 128] for h in range(4)]
            for zl in range(4):
                block = None
                for h in range(4):
                    shift = ((h - zl) * 32) % 128
                    piece = pieces[h] if shift == 0 else pltpu.roll(pieces[h], shift, 1)
                    block = piece if block is None else jnp.where(group == h, piece, block)
                blocks.append(block)
        turned = jnp.transpose(jnp.concatenate(blocks, axis=0))
        for h in range(4):
            sq[:, h, :] = turned[h * 32 : (h + 1) * 32, :]

    with jax.named_scope("barrier"):

        @pl.when(core == 0)
        def _():
            pl.semaphore_wait(barrier, NQ - 1)
            pl.semaphore_signal(told, inc=1, device_id=me + 1, device_id_type=LOGICAL)

        @pl.when(core == 1)
        def _():
            pl.semaphore_wait(told, 1)

    def plane_copy(src, dst, send, recv, k):
        peer, device = plane_peer(k)
        return pltpu.make_async_remote_copy(
            src_ref=src.at[peer], dst_ref=dst.at[q], send_sem=send, recv_sem=recv,
            device_id=device, device_id_type=LOGICAL,
        )

    def plane_all(src, dst, send, recv):
        others = pl.ds(0, NQ - 1)
        return pltpu.make_async_remote_copy(
            src_ref=src.at[others], dst_ref=dst.at[others], send_sem=send, recv_sem=recv,
            device_id=plane_peer(1)[1], device_id_type=LOGICAL,
        )

    def z_copy(src, dst, send, recv, o):
        peer, device = z_peer(o)
        return pltpu.make_async_remote_copy(
            src_ref=src.at[peer], dst_ref=dst.at[z], send_sem=send, recv_sem=recv.at[z],
            device_id=device, device_id_type=LOGICAL,
        )

    def z_arrival(src, dst, send, recv, o):
        peer, device = z_peer(o)
        return pltpu.make_async_remote_copy(
            src_ref=src.at[peer], dst_ref=dst.at[peer], send_sem=send, recv_sem=recv.at[peer],
            device_id=device, device_id_type=LOGICAL,
        )

    def z_all(src, dst, send, recv):
        others = pl.ds(0, NZ - 1)
        return pltpu.make_async_remote_copy(
            src_ref=src.at[others], dst_ref=dst.at[others], send_sem=send, recv_sem=recv.at[0],
            device_id=z_peer(1)[1], device_id_type=LOGICAL,
        )

    with jax.named_scope("plane_send"):
        for k in range(1, NQ):
            plane_copy(sq, rq, qs_sem.at[0], qr_sem.at[0], k).start()
        rq[pl.ds(q, 1)] = sq[pl.ds(q, 1)]

    def permute(n):
        ft[pl.ds(pl.multiple_of(n * 16, 16), 16), :] = gf[pl.ds(n, 16, stride=64), :].astype(jnp.bfloat16)

    with jax.named_scope("table"):
        loads[3].wait()
        for b in range(8):
            part = fl[:, :, b * 128 : (b + 1) * 128].reshape(128, 128).astype(jnp.float32)
            gf[b * 128 : (b + 1) * 128, :] = jnp.transpose(part)
        each(0, 64, permute)
    consts = [sublane_constant(v) for v in node_constants()]

    with jax.named_scope("barrier_z"):

        @pl.when(core == 1)
        def _():
            pl.semaphore_wait(barrier, 2 * (NZ - 1))
            pl.semaphore_signal(told, inc=1, device_id=me - 1, device_id_type=LOGICAL)

        @pl.when(core == 0)
        def _():
            pl.semaphore_wait(told, 1)

    with jax.named_scope("plane_wait"):
        plane_all(sq, rq, qs_sem.at[0], qr_sem.at[0]).wait_recv()
    with jax.named_scope("turn_queries"):
        gathered = jnp.concatenate([rq[:, h, :] for h in range(4)], axis=0)
        sz[...] = jnp.transpose(gathered).reshape(NZ, 8, 128)

    with jax.named_scope("z_send"):
        for distance in range(1, NZ // 2 + 1):
            for offset in sorted({NZ - distance, distance}, reverse=True):
                z_copy(sz, rz, zs_sem.at[0], zr_sem, offset).start()
        rz[pl.ds(z, 1)] = sz[pl.ds(z, 1)]

    def evaluate(peer):
        weights = []
        for sl in range(4):
            lanes = slice(sl * 128, (sl + 1) * 128)
            w0 = jnp.broadcast_to(rz[peer, sl : sl + 1, :], (8, 128))
            w1 = jnp.broadcast_to(rz[peer, 4 + sl : 5 + sl, :], (8, 128))
            basis_r = lagrange(decode(lax.shift_right_logical(w0, 16)), consts)
            basis_s = lagrange(decode(jnp.bitwise_and(w0, 65535)), consts)
            basis_t = lagrange(decode(lax.shift_right_logical(w1, 16)), consts)
            element = jnp.bitwise_and(w1, 65535)
            weights.append(
                jnp.concatenate(
                    [jnp.where(element == e, basis_r, 0.0) for e in range(16)], axis=0
                ).astype(jnp.bfloat16)
            )
            for j in range(8):
                ts[j * 8 : (j + 1) * 8, lanes] = basis_s[j : j + 1, :] * basis_t
        for half in range(2):
            pair = jnp.concatenate(weights[2 * half : 2 * half + 2], axis=1)
            lanes = slice(half * 256, (half + 1) * 256)
            partial = jnp.dot(ft[...], pair, preferred_element_type=jnp.float32)
            total = None
            for n in range(64):
                term = partial[n * 16 : (n + 1) * 16, :] * ts[n : n + 1, lanes]
                total = term if total is None else total + term
            rounded = total.astype(jnp.bfloat16)
            vs[peer, 2 * half] = rounded[:, :128]
            vs[peer, 2 * half + 1] = rounded[:, 128:]

    with jax.named_scope("own"):
        evaluate(z)
        rv[pl.ds(z, 1)] = vs[pl.ds(z, 1)]

    def remote_step(k):
        offset = nearness_to_offset(position_to_nearness(k, 10 - 4 * core))
        with jax.named_scope("z_wait"):
            z_arrival(sz, rz, zs_sem.at[0], zr_sem, offset).wait_recv()
        with jax.named_scope("evaluate"):
            evaluate(lax.rem(z + offset, NZ))
            z_copy(vs, rv, vs_sem.at[0], vr_sem, offset).start()

    each(1, NZ, remote_step)

    def turn_back(n, at):
        block = rv[lax.rem(z + ORDER[n], NZ)].reshape(64, 128).astype(jnp.float32)
        rows = jnp.transpose(jnp.concatenate([block, pltpu.roll(block, 96, 1)], axis=0))
        for half in range(2):
            srf[pl.ds(2 * at + half, 32, stride=8), :] = rows[half * 64 : half * 64 + 32, :]

    def return_group(g):
        with jax.named_scope("z_return"):
            for n in range(4 * g, 4 * g + 4):
                if n > 0:
                    z_arrival(vs, rv, vs_sem.at[0], vr_sem, ORDER[n]).wait_recv()
                turn_back(n, n - 4 * g)
        with jax.named_scope("turn_back"):
            sr[g] = srf[...].reshape(NQ, 8, 128).astype(jnp.bfloat16)
        with jax.named_scope("plane_return"):
            for k in range(1, NQ):
                plane_copy(sr.at[g], rr.at[g], ws_sem.at[g], wr_sem.at[g], k).start()
            pltpu.make_async_copy(sr.at[g, q], rr.at[g, q], own_sem.at[g]).start()

    for g in range(GROUPS):
        return_group(g)
    with jax.named_scope("drain"):
        plane_all(sq, rq, qs_sem.at[0], qr_sem.at[0]).wait_send()
        z_all(sz, rz, zs_sem.at[0], zr_sem).wait_send()
        z_all(vs, rv, vs_sem.at[0], vr_sem).wait_send()
    with jax.named_scope("plane_back"):
        for g in range(GROUPS):
            plane_all(sr.at[g], rr.at[g], ws_sem.at[g], wr_sem.at[g]).wait_recv()
            pltpu.make_async_copy(sr.at[g, q], rr.at[g, q], own_sem.at[g]).wait()
    with jax.named_scope("drain2"):
        for g in range(GROUPS):
            plane_all(sr.at[g], rr.at[g], ws_sem.at[g], wr_sem.at[g]).wait_send()


def finish(rr_hbm, out_hbm, rr, srf, rows, orf, staged, sem, in_sem):
    loads = [pltpu.make_async_copy(rr_hbm.at[g], rr.at[g], in_sem.at[g]) for g in range(GROUPS)]
    for load in loads:
        load.start()
    z = lax.div(lax.axis_index("wide"), NY)

    with jax.named_scope("widen"):
        for g in range(GROUPS):
            loads[g].wait()
            srf[g] = rr[g].reshape(NQ * 8, 128).astype(jnp.float32)
            for n in range(4):
                owner = lax.rem(z + ORDER[4 * g + n], NZ)
                for half in range(2):
                    rows[owner, half] = srf[g, pl.ds(2 * n + half, NQ, stride=8), :]
    copies = []
    for t in range(4):
        with jax.named_scope("finish"):
            for half in range(2):
                turned = jnp.transpose(jnp.concatenate([rows[t * 4 + zl, half] for zl in range(4)], axis=0))
                for n in range(8):
                    orf[t, pl.ds(half * 8 + n, 16, stride=16), :] = turned[n * 16 : (n + 1) * 16, :]
            staged[t] = orf[t].reshape(16, 16, 128).astype(jnp.bfloat16)
            copy = pltpu.make_async_copy(
                staged.at[t], out_hbm.at[:, 0, :, pl.ds(t * 128, 128)], sem.at[t]
            )
            copy.start()
            copies.append(copy)
    with jax.named_scope("store"):
        for copy in copies:
            copy.wait()


def on_device(query_coords, owner_element, pair_counts, fields):
    anywhere = pl.BlockSpec(memory_space=pl.ANY)
    vmem = pl.BlockSpec(memory_space=pltpu.VMEM)
    returned = pl.pallas_call(
        kernel,
        out_shape=jax.ShapeDtypeStruct((GROUPS, NQ, 8, 128), jnp.bfloat16),
        in_specs=[anywhere] * 4,
        out_specs=anywhere,
        scratch_shapes=[
            pltpu.VMEM((3, 1, 16, 512), jnp.float32),
            pltpu.VMEM((1, 16, 512), jnp.int32),
            pltpu.VMEM((1, 512), jnp.int32),
            pltpu.VMEM((16, 8, 1024), jnp.bfloat16),
            pltpu.VMEM((1024, 128), jnp.bfloat16),
            pltpu.VMEM((1024, 128), jnp.float32),
            pltpu.VMEM((4, 8, 512), jnp.int32),
            pltpu.VMEM((NQ, 4, 128), jnp.int32),
            pltpu.VMEM((NQ, 4, 128), jnp.int32),
            pltpu.VMEM((NZ, 8, 128), jnp.int32),
            pltpu.VMEM((NZ, 8, 128), jnp.int32),
            pltpu.VMEM((64, 512), jnp.float32),
            pltpu.VMEM((NZ, 4, 16, 128), jnp.bfloat16),
            pltpu.VMEM((NZ, 4, 16, 128), jnp.bfloat16),
            pltpu.VMEM((NQ * 8, 128), jnp.float32),
            pltpu.VMEM((GROUPS, NQ, 8, 128), jnp.bfloat16),
            pltpu.SemaphoreType.DMA((4,)),
            pltpu.SemaphoreType.DMA((1,)),
            pltpu.SemaphoreType.DMA((1,)),
            pltpu.SemaphoreType.DMA((1,)),
            pltpu.SemaphoreType.DMA((NZ,)),
            pltpu.SemaphoreType.DMA((1,)),
            pltpu.SemaphoreType.DMA((NZ,)),
            pltpu.SemaphoreType.DMA((GROUPS,)),
            pltpu.SemaphoreType.DMA((GROUPS,)),
            pltpu.SemaphoreType.DMA((GROUPS,)),
            pltpu.SemaphoreType.REGULAR,
        ],
        compiler_params=pltpu.CompilerParams(collective_id=0, has_side_effects=True),
    )(query_coords, owner_element, pair_counts, fields)
    return pl.pallas_call(
        finish,
        out_shape=jax.ShapeDtypeStruct((16, 1, 16, 512), jnp.bfloat16),
        in_specs=[anywhere],
        out_specs=anywhere,
        scratch_shapes=[
            pltpu.VMEM((GROUPS, NQ, 8, 128), jnp.bfloat16),
            pltpu.VMEM((GROUPS, NQ * 8, 128), jnp.float32),
            pltpu.VMEM((NZ, 2, NQ, 128), jnp.float32),
            pltpu.VMEM((4, 256, 128), jnp.float32),
            pltpu.VMEM((4, 16, 16, 128), jnp.bfloat16),
            pltpu.SemaphoreType.DMA((4,)),
            pltpu.SemaphoreType.DMA((GROUPS,)),
        ],
    )(returned)


def solution(mesh):
    placed = (
        P(None, ("wide", "narrow"), None, None),
        P(("wide", "narrow"), None, None),
        P(("wide", "narrow"), None),
        P(("wide", "narrow"), None, None),
    )
    return jax.shard_map(
        on_device,
        mesh=mesh,
        in_specs=placed,
        out_specs=P(None, ("wide", "narrow"), None, None),
        check_vma=False,
    )
```
